32 devices in a mesh: gx: 8 (over z, y), gy: 4 (over x, core).
Axes of the slice: x: 2, y: 2, z: 4, core: 2. Of those that a mesh axis runs over, the one named last changes fastest.
Arguments:
- populations: float32 [27, 16, 32, 128], P(None, 'gx', 'gy'), as said below
- relax: float32 [27], replicated, may hold values from 0.6 to 1.9
- solid: int32 [16, 32, 128], P('gx', 'gy'), may hold values 0 or 1
- wall_cell: int32 [8, 4, 256], P('gx', 'gy'), may hold values from 0 to 2047, as said below
- wall_normal: int32 [8, 4, 256], P('gx', 'gy'), may hold values from 0 to 5
- wall_count: int32 [8, 4], P('gx', 'gy'), may hold values from 1 to 256, as said below
- sample_ref: int32 [8, 4, 256], P('gx', 'gy'), may hold values from 0 to 255, each once within a row
- stencil_cell: int32 [8, 4, 8, 256], P('gx', 'gy'), may hold values from 0 to 2047, as said below
- stencil_weight: float32 [8, 4, 8, 256], P('gx', 'gy'), may hold values from 0 to 1, as said below
Outputs:
- read: float32 [27, 16, 32, 128], P(None, 'gx', 'gy')
The draws below stay inside these ranges and needn't reach their ends.
Inputs may be any that keep to these rules, and one draw needn't show every extreme that they name: `populations`: positive everywhere. `wall_cell`: the 256 entries of one device are distinct local cells. Slots 0 to wall_count - 1 of a device are live; some device has all 256 live. `stencil_cell`: the eight corners of a unit cube of the owner's local cells, wrapping along z only. `stencil_weight`: nonnegative trilinear weights, summing to one over the eight corners.
All inputs are finite; a program needn't handle non-finite values. No bound on the sum of `solid` on one device may be relied on, other than what follows from the above.
Results may differ from the reference program's by a relative error of at most 0.0003.
Values sent between devices are 32-bit elements; how exact they have to be, the bound alone decides.
No kernel may reach another device: no remote copies, remote signals or barrier semaphores. Data moves between devices by JAX's collectives and lax.ppermute only.
A program may use at most 64 MiB of HBM per device.

```python
import math
import jax
import jax.numpy as jnp
import numpy as np
from jax import lax

CX = 2
CY = 8
NZ = 128
SLOTS = 64
WALL = 256
NX = 16
NY = 32
N_GX = 8
N_GY = 4


def draw_populations(key, part):
    base = jax.random.fold_in(key, 101)
    steps = np.array([(a - 1, b - 1, c - 1) for a in range(3) for b in range(3) for c in range(3)]).T
    drift = np.array([0.06, 0.02, -0.02])
    projected = drift @ steps
    resting = 1.0 + 3.0 * projected + 4.5 * projected * projected - 1.5 * np.sum(drift * drift)
    shape = (27, NX, NY, NZ)
    noise = 0.12 * jnp.clip(jax.random.normal(base, shape, jnp.float32), -3.5, 3.5)
    return (jnp.asarray(resting, jnp.float32).reshape(27, 1, 1, 1) * (1.0 + noise)).astype(jnp.float32)


def draw_stencil_cell(key, part):
    grid_x = NX // CX
    grid_y = NY // CY
    shape = (grid_x, grid_y, 1, WALL)
    first, second, third = jax.random.split(jax.random.fold_in(key, 202), 3)
    base_x = jax.random.randint(first, shape, 0, CX - 1)
    base_y = jax.random.randint(second, shape, 0, CY - 1)
    base_z = jax.random.randint(third, shape, 0, NZ)
    corner = jnp.arange(8, dtype=jnp.int32).reshape(1, 1, 8, 1)
    offset_x = corner // 4
    offset_y = corner // 2 % 2
    offset_z = corner % 2
    cells = ((base_x + offset_x) * CY + base_y + offset_y) * NZ + (base_z + offset_z) % NZ
    return cells.astype(jnp.int32)


def draw_stencil_weight(key, part):
    grid_x = NX // CX
    grid_y = NY // CY
    shape = (grid_x, grid_y, 3, 1, WALL)
    base = jax.random.fold_in(key, 303)
    fraction = jax.random.uniform(base, shape, jnp.float32, 0.0, 1.0)
    corner = jnp.arange(8, dtype=jnp.int32)
    bits = jnp.stack([corner // 4, corner // 2 % 2, corner % 2]).reshape(1, 1, 3, 8, 1)
    factor = jnp.where(bits == 1, fraction, 1.0 - fraction)
    return jnp.prod(factor, axis=2).astype(jnp.float32)


def draw_wall_cell(key, part):
    grid_x = NX // CX
    grid_y = NY // CY
    keys = jax.random.split(jax.random.fold_in(key, 404), grid_x * grid_y)
    chosen = jax.vmap(lambda item: jax.random.permutation(item, CX * CY * NZ)[:WALL])(keys)
    return chosen.reshape(grid_x, grid_y, WALL).astype(jnp.int32)


def draw_wall_count(key, part):
    grid_x = NX // CX
    grid_y = NY // CY
    shifted = jax.random.randint(jax.random.fold_in(key, 505), (grid_x, grid_y), 0, 4)
    counts = jnp.right_shift(jnp.full((grid_x, grid_y), WALL, jnp.int32), shifted.astype(jnp.int32))
    counts = jnp.maximum(counts, 1).at[0, 0].set(WALL)
    return counts.astype(jnp.int32)


def plant(result, rng, smallest, top_value):
    dims = result.shape
    spot = [jax.random.randint(jax.random.fold_in(rng, axis), (), 0, dims[axis]) for axis in range(len(dims))]
    result = result.at[tuple(spot)].set(smallest)
    longest = dims.index(max(dims))
    spot[longest] = (spot[longest] + 1) % dims[longest]
    return result.at[tuple(spot)].set(top_value)


def setup_inputs(seed: int = 0) -> dict:
    arg_keys = jax.random.split(jax.random.key(seed), 10)
    populations = draw_populations(jax.random.fold_in(arg_keys[9], 71), 0)
    relax = jnp.clip(jnp.exp(jax.random.uniform(arg_keys[1], (27,), jnp.float32, math.log(0.6), math.log(1.9))), 0.6, 1.9)
    solid = plant((jax.random.randint(arg_keys[2], (NX, NY, NZ), 0, 8) < 1).astype(jnp.int32), jax.random.fold_in(arg_keys[2], 1), 0, 1)
    wall_cell = draw_wall_cell(jax.random.fold_in(arg_keys[9], 71), 0)
    wall_normal = plant(jax.random.randint(arg_keys[4], (N_GX, N_GY, WALL), 0, 6), jax.random.fold_in(arg_keys[4], 1), 0, 5).astype(jnp.int32)
    wall_count = draw_wall_count(jax.random.fold_in(arg_keys[9], 71), 0)
    sample_ref = jax.vmap(lambda own: jax.random.permutation(own, WALL))(jax.random.split(arg_keys[6], N_GX * N_GY)).reshape((N_GX, N_GY, WALL)).astype(jnp.int32)
    stencil_cell = draw_stencil_cell(jax.random.fold_in(arg_keys[9], 71), 0)
    stencil_weight = draw_stencil_weight(jax.random.fold_in(arg_keys[9], 71), 0)
    return {"populations": populations, "relax": relax, "solid": solid, "wall_cell": wall_cell, "wall_normal": wall_normal, "wall_count": wall_count, "sample_ref": sample_ref, "stencil_cell": stencil_cell, "stencil_weight": stencil_weight}


lattice_steps = [(a - 1, b - 1, c - 1) for a in range(3) for b in range(3) for c in range(3)]
wall_ratio = (1.0 / 9.0) ** (1.0 / 7.0)


def lattice():
    steps = np.array(lattice_steps).T
    single = np.where(steps == 0, 2.0 / 3.0, 1.0 / 6.0)
    weights = np.prod(single, axis=0)
    vander = np.array([[1.0, 1.0, 1.0], [-1.0, 0.0, 1.0], [1.0, 0.0, 1.0]])
    undo = np.array([[0.0, -0.5, 0.5], [1.0, 0.0, -1.0], [0.0, 0.5, 0.5]])
    moment = np.kron(np.kron(vander, vander), vander)
    inverse = np.kron(np.kron(undo, undo), undo)
    return (jnp.asarray(steps, jnp.float32), jnp.asarray(weights, jnp.float32),
            jnp.asarray(moment, jnp.float32), jnp.asarray(inverse, jnp.float32))


def moments(pops):
    steps, weights, moment, inverse = lattice()
    scaled = weights[:, None] * pops
    density = jnp.sum(scaled, axis=0)
    momentum = jnp.dot(steps, scaled, precision=lax.Precision.HIGHEST)
    return density, momentum / density[None]


def equilibrium(density, velocity):
    steps, weights, moment, inverse = lattice()
    projected = jnp.dot(steps.T, velocity, precision=lax.Precision.HIGHEST)
    speed_sq = jnp.sum(velocity * velocity, axis=0)
    return density[None] * (1.0 + 3.0 * projected + 4.5 * projected * projected - 1.5 * speed_sq[None])


def collide(pops, relax):
    steps, weights, moment, inverse = lattice()
    scaled = weights[:, None] * pops
    density, velocity = moments(pops)
    balance = weights[:, None] * equilibrium(density, velocity)
    deviation = jnp.dot(moment, scaled - balance, precision=lax.Precision.HIGHEST) * relax[:, None]
    after = scaled - jnp.dot(inverse, deviation, precision=lax.Precision.HIGHEST)
    return after / weights[:, None]


def sample_velocity(velocity, corner_cells, corner_weight):
    picked = velocity[:, corner_cells]
    return jnp.sum(picked * corner_weight[None], axis=1)


def rebuild_columns(columns, density, velocity, normal, live, picked):
    axis_index = normal // 2
    sign = (2 * (normal % 2) - 1).astype(jnp.float32)
    normal_vec = (jnp.arange(3, dtype=jnp.int32)[:, None] == axis_index[None]).astype(jnp.float32) * sign[None]
    along = jnp.sum(picked * normal_vec, axis=0)
    tangential = picked - along[None] * normal_vec
    wall_eq = equilibrium(density, wall_ratio * tangential)
    local_eq = equilibrium(density, velocity)
    return jnp.where(live[None], wall_eq + columns - local_eq, columns)


def rebuild_block(block, density, velocity, cells, normal, live, picked):
    columns = rebuild_columns(block[:, cells], density[cells], velocity[:, cells], normal, live, picked)
    return block.at[:, cells].set(columns)


def to_blocks(field):
    count = field.shape[0]
    field = field.reshape(count, N_GX, CX, N_GY, CY, NZ).transpose(1, 3, 0, 2, 4, 5)
    return field.reshape(N_GX, N_GY, count, CX * CY * NZ)


def from_blocks(blocks):
    count = blocks.shape[2]
    field = blocks.reshape(N_GX, N_GY, count, CX, CY, NZ).transpose(2, 0, 3, 1, 4, 5)
    return field.reshape(count, N_GX * CX, N_GY * CY, NZ)


def reference(populations, relax, solid, wall_cell, wall_normal, wall_count, sample_ref, stencil_cell, stencil_weight):
    blocks = to_blocks(populations)
    density_b, velocity_b = lax.map(lambda row: jax.vmap(moments)(row), blocks)
    samples = jax.vmap(jax.vmap(sample_velocity))(velocity_b, stencil_cell, stencil_weight)
    sent = samples.reshape(N_GX, N_GY, 3, N_GY, SLOTS)
    received = sent.transpose(0, 3, 2, 1, 4).reshape(N_GX, N_GY, 3, N_GY * SLOTS)
    picked = jax.vmap(jax.vmap(lambda table, where_from: table[:, where_from]))(received, sample_ref)
    live = jnp.arange(N_GY * SLOTS, dtype=jnp.int32)[None, None, :] < wall_count[:, :, None]
    rebuilt = jax.vmap(jax.vmap(rebuild_block))(blocks, density_b, velocity_b, wall_cell, wall_normal, live, picked)
    post_b = lax.map(lambda row: jax.vmap(lambda block: collide(block, relax))(row), rebuilt)
    post = from_blocks(post_b)
    outputs = []
    for direction in range(27):
        step_x, step_y, step_z = lattice_steps[direction]
        moved = jnp.roll(post[direction], (step_x, step_y, step_z), axis=(0, 1, 2))
        blocked = jnp.roll(solid, (step_x, step_y, step_z), axis=(0, 1, 2))
        outputs.append(jnp.where(blocked != 0, post[26 - direction], moved))
    return jnp.stack(outputs)
```

```python
import jax
import jax.numpy as jnp
import numpy as np
from jax import lax
from jax.experimental import pallas as pl
from jax.experimental.pallas import tpu as pltpu
from jax.sharding import PartitionSpec as P

wall_ratio = (1.0 / 9.0) ** (1.0 / 7.0)
LANES = 128
ROWS = 8
RHO, VEL, REF, AXIS, SOLID, PLANES = 27, 28, 31, 32, 33, 34
FACE = 16
ANY = pl.BlockSpec(memory_space=pl.ANY)
VMEM = pl.BlockSpec(memory_space=pltpu.VMEM)


def direction(a, b, c):
    return 9 * a + 3 * b + c


def up(n):
    return -(-n // ROWS) * ROWS


def equilibria(density, velocity, wanted):
    ux, uy, uz = velocity
    rest = density * (1.0 - 1.5 * (ux * ux + uy * uy + uz * uz))
    out = {}
    for i in wanted:
        if i in out:
            continue
        step = (i // 9 - 1, i // 3 % 3 - 1, i % 3 - 1)
        along = None
        for s, u in zip(step, (ux, uy, uz)):
            if s:
                along = (u if s > 0 else -u) if along is None else (along + u if s > 0 else along - u)
        if along is None:
            out[i] = rest
            continue
        linear = density * along
        square = rest + 4.5 * (linear * along)
        out[i] = square + 3.0 * linear
        if 26 - i in wanted:
            out[26 - i] = square - 3.0 * linear
    return out


def along_axes(values, triple):
    for stride in (1, 3, 9):
        fresh = list(values)
        for i in range(27):
            if i // stride % 3 == 0:
                fresh[i], fresh[i + stride], fresh[i + 2 * stride] = triple(
                    values[i], values[i + stride], values[i + 2 * stride]
                )
        values = fresh
    return values


def relaxed(pops, relax):
    single = (1.0 / 6.0, 2.0 / 3.0, 1.0 / 6.0)
    weight = [single[i // 9] * single[i // 3 % 3] * single[i % 3] for i in range(27)]

    def raw(m, z, p):
        s = m + p
        return s + z, p - m, s

    def undo(m0, m1, m2):
        return m2 - m1, m0 - m2, m1 + m2

    moment = along_axes([w * p for w, p in zip(weight, pops)], raw)
    density = moment[0]
    inv = 1.0 / density
    vel = [moment[9] * inv, moment[3] * inv, moment[1] * inv]
    first = [moment[9], moment[3], moment[1]]
    second = [4.5 * (j * u) for j, u in zip(first, vel)]
    rest = density - (1.0 / 3.0) * (second[0] + second[1] + second[2])
    mu, nu, ka = (1.0, 0.0, 1.0 / 3.0), (0.0, 1.0 / 3.0, 0.0), (1.0 / 3.0, 0.0, 1.0 / 3.0)
    cross = {}
    kept = []
    for i in range(27):
        p = (i // 9, i // 3 % 3, i % 3)
        eq = None
        terms = [(mu[p[0]] * mu[p[1]] * mu[p[2]], rest)]
        for d in range(3):
            o, q = [e for e in range(3) if e != d]
            terms.append((3.0 * nu[p[d]] * mu[p[o]] * mu[p[q]], first[d]))
            terms.append((ka[p[d]] * mu[p[o]] * mu[p[q]], second[d]))
            factor = 9.0 * nu[p[o]] * nu[p[q]] * mu[p[d]]
            if factor:
                if d not in cross:
                    cross[d] = first[o] * vel[q]
                terms.append((factor, cross[d]))
        for f, t in terms:
            if f:
                t = t if abs(f - 1.0) < 1e-12 else f * t
                eq = t if eq is None else eq + t
        dev = moment[i] if eq is None else moment[i] - eq
        kept.append((1.0 - relax[i]) * dev)
    back = (3.0, 1.5, 3.0)
    kept = along_axes(kept, undo)
    kept = [back[i // 9] * back[i // 3 % 3] * back[i % 3] * k for i, k in enumerate(kept)]
    return density, vel, kept


def lanes_of(table, index):
    return jnp.take_along_axis(table, index, axis=1, mode="promise_in_bounds")


def first_kernel(
    pop_h, relax_h, solid_h, cell_h, normal_h, count_h, ref_h, scell_h, sweight_h,
    up_o, down_o, sample_o, state_o,
    pop, relax, solid, cell, normal, count, ref, scell, sweight, sems,
):
    size_x = pop.shape[1]
    walls, slots = cell.shape[1], scell.shape[1]
    moves = [
        (relax_h, relax), (count_h, count), (scell_h.at[0, 0], scell), (sweight_h.at[0, 0], sweight),
        (cell_h.at[0], cell), (normal_h.at[0], normal), (ref_h.at[0], ref), (pop_h, pop), (solid_h, solid),
    ]
    copies = [pltpu.make_async_copy(s, d, sems.at[n]) for n, (s, d) in enumerate(moves)]
    for copy in copies:
        copy.start()
    for copy in copies:
        copy.wait()
    rates = [relax[i] for i in range(27)]
    velocity = []
    for x in range(size_x):
        density, vel, kept = relaxed([pop[i, x] for i in range(27)], rates)
        velocity.append(vel)
        for i in range(27):
            state_o[i, x] = kept[i]
        state_o[RHO, x] = density
        for d in range(3):
            state_o[VEL + d, x] = vel[d]
        state_o[SOLID, x] = solid[x].astype(jnp.float32)
    sub = lax.broadcasted_iota(jnp.int32, (ROWS, LANES), 0)
    for t in range(slots // LANES):
        cells = scell[:, t * LANES : (t + 1) * LANES]
        weights = sweight[:, t * LANES : (t + 1) * LANES]
        row, z = cells // LANES, cells % LANES
        low = jnp.broadcast_to(z[0:1], (ROWS, LANES))
        other = z != low
        high = jnp.max(jnp.where(other, z, 0), axis=0, keepdims=True)
        high = jnp.broadcast_to(high, (ROWS, LANES))
        w_high = jnp.where(other, weights, 0.0)
        w_low = weights - w_high
        total = [jnp.zeros((ROWS, LANES), jnp.float32) for _ in range(3)]
        for x in range(size_x):
            a_low = jnp.zeros((ROWS, LANES), jnp.float32)
            a_high = a_low
            for k in range(8):
                hit = jnp.broadcast_to(row[k : k + 1], (ROWS, LANES)) == sub + x * ROWS
                a_low += jnp.where(hit, jnp.broadcast_to(w_low[k : k + 1], (ROWS, LANES)), 0.0)
                a_high += jnp.where(hit, jnp.broadcast_to(w_high[k : k + 1], (ROWS, LANES)), 0.0)
            for d in range(3):
                total[d] += a_low * lanes_of(velocity[x][d], low) + a_high * lanes_of(velocity[x][d], high)
        for d in range(3):
            r = d * (slots // LANES) + t
            line = jnp.sum(total[d], axis=0, keepdims=True)
            for o in (up_o, down_o, sample_o):
                o[r : r + 1, :] = line
    row, z = cell[...] // LANES, cell[...] % LANES
    live = lax.broadcasted_iota(jnp.int32, (1, walls), 1) < count[0, 0]
    low = jnp.where(live, ref[...] % LANES + 1, 0).astype(jnp.float32)
    high = jnp.where(live, ref[...] // LANES * 4 + normal[...] // 2, 0).astype(jnp.float32)
    height = size_x * ROWS
    at = lax.broadcasted_iota(jnp.int32, (height, walls), 0) == jnp.broadcast_to(row, (height, walls))
    left = jnp.concatenate(
        [jnp.where(at, jnp.broadcast_to(v, (height, walls)), 0.0) for v in (low, high)], axis=0
    ).astype(jnp.bfloat16)
    hot = lax.broadcasted_iota(jnp.int32, (LANES, walls), 0) == jnp.broadcast_to(z, (LANES, walls))
    hot = jnp.where(hot, 1.0, 0.0).astype(jnp.bfloat16)
    dense = lax.dot_general(left, hot, (((1,), (1,)), ((), ())), preferred_element_type=jnp.float32)
    for x in range(size_x):
        low = dense[x * ROWS : (x + 1) * ROWS].astype(jnp.int32)
        high = dense[height + x * ROWS : height + (x + 1) * ROWS].astype(jnp.int32)
        state_o[REF, x] = ((high // 4) * LANES + low - 1).astype(jnp.float32)
        state_o[AXIS, x] = (high % 4).astype(jnp.float32)
    base = up(3 * (slots // LANES))
    for o, b, y in ((up_o, 2, ROWS - 1), (down_o, 0, 0)):
        planes = [direction(a, b, c) for a in range(3) for c in range(3)] + list(range(RHO, PLANES))
        for n, plane in enumerate(planes):
            for x in range(size_x):
                r = base + n * size_x + x
                o[r : r + 1, :] = state_o[plane, x, y : y + 1, :]


def second_kernel(own, from_below, from_above, *rest, names, peers, slots, slots_each):
    state, rest = rest[0], rest[1:]
    far, outs = rest[: peers - 3], rest[peers - 3 :]
    post_o, edge_o, even_o, odd_o = outs
    gx, gy = names
    size_x = post_o.shape[1]
    width = slots // LANES
    base = up(3 * width)
    me = lax.axis_index(gy)
    parity = lax.axis_index(gx) % 2
    tables = [(own, me), (from_below, (me + peers - 1) % peers), (from_above, (me + 1) % peers)]
    for n, table in enumerate(far):
        tables.append((table, (me + peers - (n + 2)) % peers))

    def walled(block, ref, axis, vel):
        index = jnp.maximum(ref, 0)
        source = index // slots_each
        start = block * slots_each
        tile = start // LANES
        lane = start % LANES + index % slots_each
        out = []
        for d in range(3):
            picked = jnp.zeros(ref.shape, jnp.float32)
            for table, who in tables:
                line = table[pl.ds(d * width + tile, 1), :]
                got = lanes_of(jnp.broadcast_to(line, (ROWS, LANES)), lane)
                picked = jnp.where(source == who, got, picked)
            tangential = jnp.where(axis == d, 0.0, wall_ratio * picked)
            out.append(jnp.where(ref >= 0, tangential, vel[d]))
        return out

    plus, minus, corner_plus, corner_minus = [], [], [], []
    for x in range(size_x):
        ref = state[REF, x].astype(jnp.int32)
        axis = state[AXIS, x].astype(jnp.int32)
        vel = walled(me, ref, axis, [state[VEL + d, x] for d in range(3)])
        eq = equilibria(state[RHO, x], vel, range(27))
        for i in range(27):
            value = state[i, x] + eq[i]
            post_o[i, x] = value
            if x == size_x - 1 and i >= 18:
                plus.append(value)
            if x == 0 and i < 9:
                minus.append(value)
    plus.append(state[SOLID, size_x - 1])
    minus.append(state[SOLID, 0])
    sub = lax.broadcasted_iota(jnp.int32, (ROWS, LANES), 0)
    for side, (table, b, block) in enumerate(
        ((from_below, 2, (me + peers - 1) % peers), (from_above, 0, (me + 1) % peers))
    ):
        def plane(n):
            rows = [table[base + n * size_x + x : base + n * size_x + x + 1, :] for x in range(size_x)]
            tile = jnp.broadcast_to(rows[0], (ROWS, LANES))
            for x in range(1, size_x):
                tile = jnp.where(sub == x, jnp.broadcast_to(rows[x], (ROWS, LANES)), tile)
            return tile

        ref = plane(13).astype(jnp.int32)
        axis = plane(14).astype(jnp.int32)
        vel = walled(block, ref, axis, [plane(10 + d) for d in range(3)])
        wanted = [direction(a, b, c) for a in range(3) for c in range(3)]
        eq = equilibria(plane(9), vel, wanted)
        for n, i in enumerate(wanted):
            value = plane(n) + eq[i]
            r = (side * 10 + n) * size_x
            edge_o[r : r + size_x, :] = value[:size_x]
            if i >= 18:
                corner_plus.append(value[size_x - 1 : size_x])
            if i < 9:
                corner_minus.append(value[0:1])
        solid = plane(15)
        r = (side * 10 + 9) * size_x
        edge_o[r : r + size_x, :] = solid[:size_x]
        corner_plus.append(solid[size_x - 1 : size_x])
        corner_minus.append(solid[0:1])
    for n in range(10):
        even_o[n] = jnp.where(parity == 0, plus[n], minus[n])
        odd_o[n] = jnp.where(parity == 0, minus[n], plus[n])
    for n in range(8):
        even_o[10, n : n + 1, :] = jnp.where(parity == 0, corner_plus[n], corner_minus[n])
        odd_o[10, n : n + 1, :] = jnp.where(parity == 0, corner_minus[n], corner_plus[n])


def third_kernel(post, edge, state, even, odd, out_h, out, sems, *, names):
    gx, gy = names
    size_x = post.shape[1]
    parity = lax.axis_index(gx) % 2
    sub = lax.broadcasted_iota(jnp.int32, (ROWS, LANES), 0)

    def below(n):
        return jnp.where(parity == 0, odd[n], even[n])

    def above(n):
        return jnp.where(parity == 0, even[n], odd[n])

    corners = {-1: below(10), size_x: above(10)}

    def shifted(tile, row, step_y):
        if step_y == 0:
            return tile
        rolled = pltpu.roll(tile, step_y % ROWS, 0)
        return jnp.where(sub == (0 if step_y > 0 else ROWS - 1), jnp.broadcast_to(row, (ROWS, LANES)), rolled)

    def source(x, step_y, n_face, n_edge, n_corner, inside):
        side = 0 if step_y > 0 else 1
        if 0 <= x < size_x:
            tile = inside(x)
            r = (side * 10 + n_edge) * size_x + x
            row = edge[r : r + 1, :] if step_y else None
        else:
            tile = below(n_face) if x < 0 else above(n_face)
            row = corners[x][side * 4 + n_corner : side * 4 + n_corner + 1] if step_y else None
        return shifted(tile, row, step_y)

    copies = []
    for a in range(3):
        for b in range(3):
            for x in range(size_x):
                from_x, step_y = x - (a - 1), b - 1
                wall = source(from_x, step_y, 9, 9, 3, lambda q: state[SOLID, q])
                for c in range(3):
                    i = direction(a, b, c)
                    moved = source(from_x, step_y, 3 * b + c, 3 * a + c, c, lambda q: post[i, q])
                    solid = wall
                    if c != 1:
                        moved = pltpu.roll(moved, (c - 1) % LANES, 1)
                        solid = pltpu.roll(wall, (c - 1) % LANES, 1)
                    out[i, x] = jnp.where(solid > 0.5, post[26 - i, x], moved)
        copy = pltpu.make_async_copy(out.at[pl.ds(9 * a, 9)], out_h.at[pl.ds(9 * a, 9)], sems.at[a])
        copy.start()
        copies.append(copy)
    for copy in copies:
        copy.wait()


def local(
    populations, relax, solid, wall_cell, wall_normal, wall_count, sample_ref, stencil_cell, stencil_weight
):
    chans, size_x, size_y, size_z = populations.shape
    walls, slots = wall_cell.shape[-1], stencil_cell.shape[-1]
    devices, peers = lax.axis_size("gx"), lax.axis_size("gy")
    slots_each = slots // peers
    if (size_y, size_z) != (ROWS, LANES) or walls % LANES or slots % LANES:
        raise ValueError("unsupported block")
    if LANES % slots_each or devices % 2 or peers < 4:
        raise ValueError("unsupported mesh")
    f32 = jnp.float32
    lines = up(3 * (slots // LANES))
    face = (lines + FACE * size_x, LANES)
    block = (size_x, ROWS, LANES)
    up_face, down_face, samples, state = pl.pallas_call(
        first_kernel,
        out_shape=[
            jax.ShapeDtypeStruct(face, f32),
            jax.ShapeDtypeStruct(face, f32),
            jax.ShapeDtypeStruct((lines, LANES), f32),
            jax.ShapeDtypeStruct((PLANES, *block), f32),
        ],
        in_specs=[ANY] * 9,
        out_specs=[VMEM] * 4,
        scratch_shapes=[
            pltpu.VMEM(populations.shape, f32),
            pltpu.SMEM(relax.shape, f32),
            pltpu.VMEM(block, jnp.int32),
            pltpu.VMEM((1, walls), jnp.int32),
            pltpu.VMEM((1, walls), jnp.int32),
            pltpu.SMEM((1, 1), jnp.int32),
            pltpu.VMEM((1, walls), jnp.int32),
            pltpu.VMEM((8, slots), jnp.int32),
            pltpu.VMEM((8, slots), f32),
            pltpu.SemaphoreType.DMA((9,)),
        ],
        name="first",
    )(populations, relax, solid, wall_cell, wall_normal, wall_count, sample_ref, stencil_cell, stencil_weight)

    def shift(value, by):
        return lax.ppermute(value, "gy", [(i, (i + by) % peers) for i in range(peers)])

    from_below = shift(up_face, 1)
    from_above = shift(down_face, peers - 1)
    far = [shift(samples, n) for n in range(2, peers - 1)]
    names = ("gx", "gy")
    post, edge, even, odd = pl.pallas_call(
        lambda *refs: second_kernel(*refs, names=names, peers=peers, slots=slots, slots_each=slots_each),
        out_shape=[
            jax.ShapeDtypeStruct(populations.shape, f32),
            jax.ShapeDtypeStruct((up(20 * size_x), LANES), f32),
            jax.ShapeDtypeStruct((11, ROWS, LANES), f32),
            jax.ShapeDtypeStruct((11, ROWS, LANES), f32),
        ],
        in_specs=[VMEM] * (4 + len(far)),
        out_specs=[VMEM] * 4,
        name="second",
    )(samples, from_below, from_above, state, *far)
    swap_even = [(i, i ^ 1) for i in range(devices)]
    swap_odd = [(i, ((i - 1) ^ 1) + 1) for i in range(devices)]
    swap_odd = [(i, j % devices) for i, j in swap_odd]
    got_odd = lax.ppermute(odd, "gx", swap_odd)
    got_even = lax.ppermute(even, "gx", swap_even)
    return pl.pallas_call(
        lambda *refs: third_kernel(*refs, names=names),
        out_shape=jax.ShapeDtypeStruct(populations.shape, f32),
        in_specs=[VMEM] * 5,
        out_specs=ANY,
        scratch_shapes=[pltpu.VMEM(populations.shape, f32), pltpu.SemaphoreType.DMA((3,))],
        name="third",
    )(post, edge, state, got_even, got_odd)


def solution(mesh):
    return jax.shard_map(
        local,
        mesh=mesh,
        in_specs=(
            P(None, "gx", "gy", None),
            P(),
            P("gx", "gy", None),
            P("gx", "gy", None),
            P("gx", "gy", None),
            P("gx", "gy"),
            P("gx", "gy", None),
            P("gx", "gy", None, None),
            P("gx", "gy", None, None),
        ),
        out_specs=P(None, "gx", "gy", None),
        check_vma=False,
    )
```

```python
import jax
import jax.numpy as jnp
import numpy as np
from jax import lax
from jax.experimental import pallas as pl
from jax.experimental.pallas import tpu as pltpu
from jax.sharding import PartitionSpec as P

wall_ratio = (1.0 / 9.0) ** (1.0 / 7.0)
LANES = 128
ROWS = 8
RHO, VEL, REF, AXIS, SOLID, PLANES = 27, 28, 31, 32, 33, 34
FACE = 16
HBM = pl.BlockSpec(memory_space=pltpu.HBM)
VMEM = pl.BlockSpec(memory_space=pltpu.VMEM)
GRANT = 4 * 1024 * 1024


def direction(a, b, c):
    return 9 * a + 3 * b + c


def up(n):
    return -(-n // ROWS) * ROWS


def equilibria(density, velocity, wanted):
    ux, uy, uz = velocity
    rest = density * (1.0 - 1.5 * (ux * ux + uy * uy + uz * uz))
    out = {}
    for i in wanted:
        if i in out:
            continue
        step = (i // 9 - 1, i // 3 % 3 - 1, i % 3 - 1)
        along = None
        for s, u in zip(step, (ux, uy, uz)):
            if s:
                along = (u if s > 0 else -u) if along is None else (along + u if s > 0 else along - u)
        if along is None:
            out[i] = rest
            continue
        linear = density * along
        square = rest + 4.5 * (linear * along)
        out[i] = square + 3.0 * linear
        if 26 - i in wanted:
            out[26 - i] = square - 3.0 * linear
    return out


def along_axes(values, triple):
    for stride in (1, 3, 9):
        fresh = list(values)
        for i in range(27):
            if i // stride % 3 == 0:
                fresh[i], fresh[i + stride], fresh[i + 2 * stride] = triple(
                    values[i], values[i + stride], values[i + 2 * stride]
                )
        values = fresh
    return values


def relaxed(pops, relax):
    single = (1.0 / 6.0, 2.0 / 3.0, 1.0 / 6.0)
    weight = [single[i // 9] * single[i // 3 % 3] * single[i % 3] for i in range(27)]

    def raw(m, z, p):
        s = m + p
        return s + z, p - m, s

    def undo(m0, m1, m2):
        return m2 - m1, m0 - m2, m1 + m2

    moment = along_axes([w * p for w, p in zip(weight, pops)], raw)
    density = moment[0]
    inv = 1.0 / density
    vel = [moment[9] * inv, moment[3] * inv, moment[1] * inv]
    first = [moment[9], moment[3], moment[1]]
    second = [4.5 * (j * u) for j, u in zip(first, vel)]
    rest = density - (1.0 / 3.0) * (second[0] + second[1] + second[2])
    mu, nu, ka = (1.0, 0.0, 1.0 / 3.0), (0.0, 1.0 / 3.0, 0.0), (1.0 / 3.0, 0.0, 1.0 / 3.0)
    cross = {}
    kept = []
    for i in range(27):
        p = (i // 9, i // 3 % 3, i % 3)
        eq = None
        terms = [(mu[p[0]] * mu[p[1]] * mu[p[2]], rest)]
        for d in range(3):
            o, q = [e for e in range(3) if e != d]
            terms.append((3.0 * nu[p[d]] * mu[p[o]] * mu[p[q]], first[d]))
            terms.append((ka[p[d]] * mu[p[o]] * mu[p[q]], second[d]))
            factor = 9.0 * nu[p[o]] * nu[p[q]] * mu[p[d]]
            if factor:
                if d not in cross:
                    cross[d] = first[o] * vel[q]
                terms.append((factor, cross[d]))
        for f, t in terms:
            if f:
                t = t if abs(f - 1.0) < 1e-12 else f * t
                eq = t if eq is None else eq + t
        dev = moment[i] if eq is None else moment[i] - eq
        kept.append((1.0 - relax[i]) * dev)
    back = (3.0, 1.5, 3.0)
    kept = along_axes(kept, undo)
    kept = [back[i // 9] * back[i // 3 % 3] * back[i % 3] * k for i, k in enumerate(kept)]
    return density, vel, kept


def lanes_of(table, index):
    return jnp.take_along_axis(table, index, axis=1, mode="promise_in_bounds")


def first_kernel(
    pop_h, relax_h, solid_h, cell_h, normal_h, count_h, ref_h, scell_h, sweight_h,
    up_o, down_o, sample_o, state_o,
    pop, relax, solid, cell, normal, count, ref, scell, sweight, sems,
):
    size_x = pop.shape[1]
    walls, slots = cell.shape[1], scell.shape[1]
    moves = [
        (relax_h, relax), (count_h, count), (scell_h.at[0, 0], scell), (sweight_h.at[0, 0], sweight),
        (cell_h.at[0], cell), (normal_h.at[0], normal), (ref_h.at[0], ref), (pop_h, pop), (solid_h, solid),
    ]
    copies = [pltpu.make_async_copy(s, d, sems.at[n]) for n, (s, d) in enumerate(moves)]
    for copy in copies:
        copy.start()
    for copy in copies:
        copy.wait()
    rates = [relax[i] for i in range(27)]
    velocity = []
    for x in range(size_x):
        density, vel, kept = relaxed([pop[i, x] for i in range(27)], rates)
        velocity.append(vel)
        for i in range(27):
            state_o[i, x] = kept[i]
        state_o[RHO, x] = density
        for d in range(3):
            state_o[VEL + d, x] = vel[d]
        state_o[SOLID, x] = solid[x].astype(jnp.float32)
    sub = lax.broadcasted_iota(jnp.int32, (ROWS, LANES), 0)
    for t in range(slots // LANES):
        cells = scell[:, t * LANES : (t + 1) * LANES]
        weights = sweight[:, t * LANES : (t + 1) * LANES]
        row, z = cells // LANES, cells % LANES
        low = jnp.broadcast_to(z[0:1], (ROWS, LANES))
        other = z != low
        high = jnp.max(jnp.where(other, z, 0), axis=0, keepdims=True)
        high = jnp.broadcast_to(high, (ROWS, LANES))
        w_high = jnp.where(other, weights, 0.0)
        w_low = weights - w_high
        total = [jnp.zeros((ROWS, LANES), jnp.float32) for _ in range(3)]
        for x in range(size_x):
            a_low = jnp.zeros((ROWS, LANES), jnp.float32)
            a_high = a_low
            for k in range(8):
                hit = jnp.broadcast_to(row[k : k + 1], (ROWS, LANES)) == sub + x * ROWS
                a_low += jnp.where(hit, jnp.broadcast_to(w_low[k : k + 1], (ROWS, LANES)), 0.0)
                a_high += jnp.where(hit, jnp.broadcast_to(w_high[k : k + 1], (ROWS, LANES)), 0.0)
            for d in range(3):
                total[d] += a_low * lanes_of(velocity[x][d], low) + a_high * lanes_of(velocity[x][d], high)
        for d in range(3):
            r = d * (slots // LANES) + t
            line = jnp.sum(total[d], axis=0, keepdims=True)
            for o in (up_o, down_o, sample_o):
                o[r : r + 1, :] = line
    row, z = cell[...] // LANES, cell[...] % LANES
    live = lax.broadcasted_iota(jnp.int32, (1, walls), 1) < count[0, 0]
    low = jnp.where(live, ref[...] % LANES + 1, 0).astype(jnp.float32)
    high = jnp.where(live, ref[...] // LANES * 4 + normal[...] // 2, 0).astype(jnp.float32)
    height = size_x * ROWS
    at = lax.broadcasted_iota(jnp.int32, (height, walls), 0) == jnp.broadcast_to(row, (height, walls))
    left = jnp.concatenate(
        [jnp.where(at, jnp.broadcast_to(v, (height, walls)), 0.0) for v in (low, high)], axis=0
    ).astype(jnp.bfloat16)
    hot = lax.broadcasted_iota(jnp.int32, (LANES, walls), 0) == jnp.broadcast_to(z, (LANES, walls))
    hot = jnp.where(hot, 1.0, 0.0).astype(jnp.bfloat16)
    dense = lax.dot_general(left, hot, (((1,), (1,)), ((), ())), preferred_element_type=jnp.float32)
    for x in range(size_x):
        low = dense[x * ROWS : (x + 1) * ROWS].astype(jnp.int32)
        high = dense[height + x * ROWS : height + (x + 1) * ROWS].astype(jnp.int32)
        state_o[REF, x] = ((high // 4) * LANES + low - 1).astype(jnp.float32)
        state_o[AXIS, x] = (high % 4).astype(jnp.float32)
    base = up(3 * (slots // LANES))
    for o, b, y in ((up_o, 2, ROWS - 1), (down_o, 0, 0)):
        planes = [direction(a, b, c) for a in range(3) for c in range(3)] + list(range(RHO, PLANES))
        for n, plane in enumerate(planes):
            for x in range(size_x):
                r = base + n * size_x + x
                o[r : r + 1, :] = state_o[plane, x, y : y + 1, :]


def second_kernel(own, from_below, from_above, *rest, names, peers, slots, slots_each):
    state, rest = rest[0], rest[1:]
    far, outs = rest[: peers - 3], rest[peers - 3 :]
    post_o, edge_o, even_o, odd_o = outs
    gx, gy = names
    size_x = post_o.shape[1]
    width = slots // LANES
    base = up(3 * width)
    me = lax.axis_index(gy)
    parity = lax.axis_index(gx) % 2
    tables = [(own, me), (from_below, (me + peers - 1) % peers), (from_above, (me + 1) % peers)]
    for n, table in enumerate(far):
        tables.append((table, (me + peers - (n + 2)) % peers))

    def walled(block, ref, axis, vel):
        index = jnp.maximum(ref, 0)
        source = index // slots_each
        start = block * slots_each
        tile = start // LANES
        lane = start % LANES + index % slots_each
        out = []
        for d in range(3):
            picked = jnp.zeros(ref.shape, jnp.float32)
            for table, who in tables:
                line = table[pl.ds(d * width + tile, 1), :]
                got = lanes_of(jnp.broadcast_to(line, (ROWS, LANES)), lane)
                picked = jnp.where(source == who, got, picked)
            tangential = jnp.where(axis == d, 0.0, wall_ratio * picked)
            out.append(jnp.where(ref >= 0, tangential, vel[d]))
        return out

    plus, minus, corner_plus, corner_minus = [], [], [], []
    for x in range(size_x):
        ref = state[REF, x].astype(jnp.int32)
        axis = state[AXIS, x].astype(jnp.int32)
        vel = walled(me, ref, axis, [state[VEL + d, x] for d in range(3)])
        eq = equilibria(state[RHO, x], vel, range(27))
        for i in range(27):
            value = state[i, x] + eq[i]
            post_o[i, x] = value
            if x == size_x - 1 and i >= 18:
                plus.append(value)
            if x == 0 and i < 9:
                minus.append(value)
    plus.append(state[SOLID, size_x - 1])
    minus.append(state[SOLID, 0])
    sub = lax.broadcasted_iota(jnp.int32, (ROWS, LANES), 0)
    for side, (table, b, block) in enumerate(
        ((from_below, 2, (me + peers - 1) % peers), (from_above, 0, (me + 1) % peers))
    ):
        def plane(n):
            rows = [table[base + n * size_x + x : base + n * size_x + x + 1, :] for x in range(size_x)]
            tile = jnp.broadcast_to(rows[0], (ROWS, LANES))
            for x in range(1, size_x):
                tile = jnp.where(sub == x, jnp.broadcast_to(rows[x], (ROWS, LANES)), tile)
            return tile

        ref = plane(13).astype(jnp.int32)
        axis = plane(14).astype(jnp.int32)
        vel = walled(block, ref, axis, [plane(10 + d) for d in range(3)])
        wanted = [direction(a, b, c) for a in range(3) for c in range(3)]
        eq = equilibria(plane(9), vel, wanted)
        for n, i in enumerate(wanted):
            value = plane(n) + eq[i]
            r = (side * 10 + n) * size_x
            edge_o[r : r + size_x, :] = value[:size_x]
            if i >= 18:
                corner_plus.append(value[size_x - 1 : size_x])
            if i < 9:
                corner_minus.append(value[0:1])
        solid = plane(15)
        r = (side * 10 + 9) * size_x
        edge_o[r : r + size_x, :] = solid[:size_x]
        corner_plus.append(solid[size_x - 1 : size_x])
        corner_minus.append(solid[0:1])
    for n in range(10):
        even_o[n] = jnp.where(parity == 0, plus[n], minus[n])
        odd_o[n] = jnp.where(parity == 0, minus[n], plus[n])
    for n in range(8):
        even_o[10, n : n + 1, :] = jnp.where(parity == 0, corner_plus[n], corner_minus[n])
        odd_o[10, n : n + 1, :] = jnp.where(parity == 0, corner_minus[n], corner_plus[n])


def third_kernel(post, edge, state, even, odd, out_h, out, sems, *, names):
    gx, gy = names
    size_x = post.shape[1]
    parity = lax.axis_index(gx) % 2
    sub = lax.broadcasted_iota(jnp.int32, (ROWS, LANES), 0)

    def below(n):
        return jnp.where(parity == 0, odd[n], even[n])

    def above(n):
        return jnp.where(parity == 0, even[n], odd[n])

    corners = {-1: below(10), size_x: above(10)}

    def shifted(tile, row, step_y):
        if step_y == 0:
            return tile
        rolled = pltpu.roll(tile, step_y % ROWS, 0)
        return jnp.where(sub == (0 if step_y > 0 else ROWS - 1), jnp.broadcast_to(row, (ROWS, LANES)), rolled)

    def source(x, step_y, n_face, n_edge, n_corner, inside):
        side = 0 if step_y > 0 else 1
        if 0 <= x < size_x:
            tile = inside(x)
            r = (side * 10 + n_edge) * size_x + x
            row = edge[r : r + 1, :] if step_y else None
        else:
            tile = below(n_face) if x < 0 else above(n_face)
            row = corners[x][side * 4 + n_corner : side * 4 + n_corner + 1] if step_y else None
        return shifted(tile, row, step_y)

    copies = []
    for a in range(3):
        for b in range(3):
            for x in range(size_x):
                from_x, step_y = x - (a - 1), b - 1
                wall = source(from_x, step_y, 9, 9, 3, lambda q: state[SOLID, q])
                for c in range(3):
                    i = direction(a, b, c)
                    moved = source(from_x, step_y, 3 * b + c, 3 * a + c, c, lambda q: post[i, q])
                    solid = wall
                    if c != 1:
                        moved = pltpu.roll(moved, (c - 1) % LANES, 1)
                        solid = pltpu.roll(wall, (c - 1) % LANES, 1)
                    out[i, x] = jnp.where(solid > 0.5, post[26 - i, x], moved)
        copy = pltpu.make_async_copy(out.at[pl.ds(9 * a, 9)], out_h.at[pl.ds(9 * a, 9)], sems.at[a])
        copy.start()
        copies.append(copy)
    for copy in copies:
        copy.wait()


def local(
    populations, relax, solid, wall_cell, wall_normal, wall_count, sample_ref, stencil_cell, stencil_weight
):
    chans, size_x, size_y, size_z = populations.shape
    walls, slots = wall_cell.shape[-1], stencil_cell.shape[-1]
    devices, peers = lax.axis_size("gx"), lax.axis_size("gy")
    slots_each = slots // peers
    if (size_y, size_z) != (ROWS, LANES) or walls % LANES or slots % LANES:
        raise ValueError("unsupported block")
    if LANES % slots_each or devices % 2 or peers < 4:
        raise ValueError("unsupported mesh")
    f32 = jnp.float32
    lines = up(3 * (slots // LANES))
    face = (lines + FACE * size_x, LANES)
    block = (size_x, ROWS, LANES)
    up_face, down_face, samples, state = pl.pallas_call(
        first_kernel,
        out_shape=[
            jax.ShapeDtypeStruct(face, f32),
            jax.ShapeDtypeStruct(face, f32),
            jax.ShapeDtypeStruct((lines, LANES), f32),
            jax.ShapeDtypeStruct((PLANES, *block), f32),
        ],
        in_specs=[HBM] * 9,
        out_specs=[VMEM] * 4,
        scratch_shapes=[
            pltpu.VMEM(populations.shape, f32),
            pltpu.SMEM(relax.shape, f32),
            pltpu.VMEM(block, jnp.int32),
            pltpu.VMEM((1, walls), jnp.int32),
            pltpu.VMEM((1, walls), jnp.int32),
            pltpu.SMEM((1, 1), jnp.int32),
            pltpu.VMEM((1, walls), jnp.int32),
            pltpu.VMEM((8, slots), jnp.int32),
            pltpu.VMEM((8, slots), f32),
            pltpu.SemaphoreType.DMA((9,)),
        ],
        compiler_params=pltpu.CompilerParams(vmem_limit_bytes=GRANT),
        name="first",
    )(
        *(
            v if v is wall_count else pltpu.with_memory_space_constraint(v, pltpu.HBM)
            for v in (
                populations, relax, solid, wall_cell, wall_normal, wall_count, sample_ref, stencil_cell, stencil_weight
            )
        )
    )

    def shift(value, by):
        return lax.ppermute(value, "gy", [(i, (i + by) % peers) for i in range(peers)])

    from_below = shift(up_face, 1)
    from_above = shift(down_face, peers - 1)
    far = [shift(samples, n) for n in range(2, peers - 1)]
    names = ("gx", "gy")
    post, edge, even, odd = pl.pallas_call(
        lambda *refs: second_kernel(*refs, names=names, peers=peers, slots=slots, slots_each=slots_each),
        out_shape=[
            jax.ShapeDtypeStruct(populations.shape, f32),
            jax.ShapeDtypeStruct((up(20 * size_x), LANES), f32),
            jax.ShapeDtypeStruct((11, ROWS, LANES), f32),
            jax.ShapeDtypeStruct((11, ROWS, LANES), f32),
        ],
        in_specs=[VMEM] * (4 + len(far)),
        out_specs=[VMEM] * 4,
        compiler_params=pltpu.CompilerParams(vmem_limit_bytes=GRANT),
        name="second",
    )(samples, from_below, from_above, state, *far)
    swap_even = [(i, i ^ 1) for i in range(devices)]
    swap_odd = [(i, ((i - 1) ^ 1) + 1) for i in range(devices)]
    swap_odd = [(i, j % devices) for i, j in swap_odd]
    got_odd = lax.ppermute(odd, "gx", swap_odd)
    got_even = lax.ppermute(even, "gx", swap_even)
    return pl.pallas_call(
        lambda *refs: third_kernel(*refs, names=names),
        out_shape=jax.ShapeDtypeStruct(populations.shape, f32),
        in_specs=[VMEM] * 5,
        out_specs=HBM,
        scratch_shapes=[pltpu.VMEM(populations.shape, f32), pltpu.SemaphoreType.DMA((3,))],
        compiler_params=pltpu.CompilerParams(vmem_limit_bytes=GRANT),
        name="third",
    )(post, edge, state, got_even, got_odd)


def solution(mesh):
    return jax.shard_map(
        local,
        mesh=mesh,
        in_specs=(
            P(None, "gx", "gy", None),
            P(),
            P("gx", "gy", None),
            P("gx", "gy", None),
            P("gx", "gy", None),
            P("gx", "gy"),
            P("gx", "gy", None),
            P("gx", "gy", None, None),
            P("gx", "gy", None, None),
        ),
        out_specs=P(None, "gx", "gy", None),
        check_vma=False,
    )
```

```python
import jax
import jax.numpy as jnp
from jax import lax
from jax.experimental import pallas as pl
from jax.experimental.pallas import tpu as pltpu
from jax.sharding import PartitionSpec as P


wall_ratio = (1.0 / 9.0) ** (1.0 / 7.0)
LANES = 128
ROWS = 8
RHO, VEL, REF, AXIS, SOLID, PLANES = 27, 28, 31, 32, 33, 34
FACE = 16
HBM = pl.BlockSpec(memory_space=pltpu.HBM)
VMEM = pl.BlockSpec(memory_space=pltpu.VMEM)
GRANT = 4 * 1024 * 1024


def direction(a, b, c):
    return 9 * a + 3 * b + c


def up(n):
    return -(-n // ROWS) * ROWS


def equilibria(density, velocity, wanted):
    ux, uy, uz = velocity
    rest = density * (1.0 - 1.5 * (ux * ux + uy * uy + uz * uz))
    out = {}
    for i in wanted:
        if i in out:
            continue
        step = (i // 9 - 1, i // 3 % 3 - 1, i % 3 - 1)
        along = None
        for s, u in zip(step, (ux, uy, uz)):
            if s:
                along = (u if s > 0 else -u) if along is None else (along + u if s > 0 else along - u)
        if along is None:
            out[i] = rest
            continue
        linear = density * along
        square = rest + 4.5 * (linear * along)
        out[i] = square + 3.0 * linear
        if 26 - i in wanted:
            out[26 - i] = square - 3.0 * linear
    return out


def along_axes(values, triple):
    for stride in (1, 3, 9):
        fresh = list(values)
        for i in range(27):
            if i // stride % 3 == 0:
                fresh[i], fresh[i + stride], fresh[i + 2 * stride] = triple(
                    values[i], values[i + stride], values[i + 2 * stride]
                )
        values = fresh
    return values


def relaxed(pops, relax):
    single = (1.0 / 6.0, 2.0 / 3.0, 1.0 / 6.0)
    weight = [single[i // 9] * single[i // 3 % 3] * single[i % 3] for i in range(27)]

    def raw(m, z, p):
        s = m + p
        return s + z, p - m, s

    def undo(m0, m1, m2):
        return m2 - m1, m0 - m2, m1 + m2

    moment = along_axes([w * p for w, p in zip(weight, pops)], raw)
    density = moment[0]
    inv = 1.0 / density
    vel = [moment[9] * inv, moment[3] * inv, moment[1] * inv]
    first = [moment[9], moment[3], moment[1]]
    second = [4.5 * (j * u) for j, u in zip(first, vel)]
    rest = density - (1.0 / 3.0) * (second[0] + second[1] + second[2])
    mu, nu, ka = (1.0, 0.0, 1.0 / 3.0), (0.0, 1.0 / 3.0, 0.0), (1.0 / 3.0, 0.0, 1.0 / 3.0)
    cross = {}
    kept = []
    for i in range(27):
        p = (i // 9, i // 3 % 3, i % 3)
        eq = None
        terms = [(mu[p[0]] * mu[p[1]] * mu[p[2]], rest)]
        for d in range(3):
            o, q = [e for e in range(3) if e != d]
            terms.append((3.0 * nu[p[d]] * mu[p[o]] * mu[p[q]], first[d]))
            terms.append((ka[p[d]] * mu[p[o]] * mu[p[q]], second[d]))
            factor = 9.0 * nu[p[o]] * nu[p[q]] * mu[p[d]]
            if factor:
                if d not in cross:
                    cross[d] = first[o] * vel[q]
                terms.append((factor, cross[d]))
        for f, t in terms:
            if f:
                t = t if abs(f - 1.0) < 1e-12 else f * t
                eq = t if eq is None else eq + t
        dev = moment[i] if eq is None else moment[i] - eq
        kept.append((1.0 - relax[i]) * dev)
    back = (3.0, 1.5, 3.0)
    kept = along_axes(kept, undo)
    kept = [back[i // 9] * back[i // 3 % 3] * back[i % 3] * k for i, k in enumerate(kept)]
    return density, vel, kept


def lanes_of(table, index):
    return jnp.take_along_axis(table, index, axis=1, mode="promise_in_bounds")


def first_kernel(
    pop_h, relax_h, solid_h, cell_h, normal_h, count_h, ref_h, scell_h, sweight_h,
    even_o, odd_o, sample_o, state_o,
    pop, relax, solid, cell, normal, count, ref, scell, sweight, sems, *, gy,
):
    size_x = pop.shape[1]
    walls, slots = cell.shape[1], scell.shape[1]
    moves = [
        (relax_h, relax), (count_h, count), (scell_h.at[0, 0], scell), (sweight_h.at[0, 0], sweight),
        (cell_h.at[0], cell), (normal_h.at[0], normal), (ref_h.at[0], ref), (pop_h, pop), (solid_h, solid),
    ]
    copies = [pltpu.make_async_copy(s, d, sems.at[n]) for n, (s, d) in enumerate(moves)]
    for copy in copies:
        copy.start()
    for copy in copies:
        copy.wait()
    rates = [relax[i] for i in range(27)]
    velocity = []
    for x in range(size_x):
        density, vel, kept = relaxed([pop[i, x] for i in range(27)], rates)
        velocity.append(vel)
        for i in range(27):
            state_o[i, x] = kept[i]
        state_o[RHO, x] = density
        for d in range(3):
            state_o[VEL + d, x] = vel[d]
        state_o[SOLID, x] = solid[x].astype(jnp.float32)
    sub = lax.broadcasted_iota(jnp.int32, (ROWS, LANES), 0)
    for t in range(slots // LANES):
        cells = scell[:, t * LANES : (t + 1) * LANES]
        weights = sweight[:, t * LANES : (t + 1) * LANES]
        row, z = cells // LANES, cells % LANES
        low = jnp.broadcast_to(z[0:1], (ROWS, LANES))
        other = z != low
        high = jnp.max(jnp.where(other, z, 0), axis=0, keepdims=True)
        high = jnp.broadcast_to(high, (ROWS, LANES))
        w_high = jnp.where(other, weights, 0.0)
        w_low = weights - w_high
        total = [jnp.zeros((ROWS, LANES), jnp.float32) for _ in range(3)]
        for x in range(size_x):
            a_low = jnp.zeros((ROWS, LANES), jnp.float32)
            a_high = a_low
            for k in range(8):
                hit = jnp.broadcast_to(row[k : k + 1], (ROWS, LANES)) == sub + x * ROWS
                a_low += jnp.where(hit, jnp.broadcast_to(w_low[k : k + 1], (ROWS, LANES)), 0.0)
                a_high += jnp.where(hit, jnp.broadcast_to(w_high[k : k + 1], (ROWS, LANES)), 0.0)
            for d in range(3):
                total[d] += a_low * lanes_of(velocity[x][d], low) + a_high * lanes_of(velocity[x][d], high)
        for d in range(3):
            r = d * (slots // LANES) + t
            line = jnp.sum(total[d], axis=0, keepdims=True)
            for o in (even_o, odd_o, sample_o):
                o[r : r + 1, :] = line
    row, z = cell[...] // LANES, cell[...] % LANES
    live = lax.broadcasted_iota(jnp.int32, (1, walls), 1) < count[0, 0]
    low = jnp.where(live, ref[...] % LANES + 1, 0).astype(jnp.float32)
    high = jnp.where(live, ref[...] // LANES * 4 + normal[...] // 2, 0).astype(jnp.float32)
    height = size_x * ROWS
    at = lax.broadcasted_iota(jnp.int32, (height, walls), 0) == jnp.broadcast_to(row, (height, walls))
    left = jnp.concatenate(
        [jnp.where(at, jnp.broadcast_to(v, (height, walls)), 0.0) for v in (low, high)], axis=0
    ).astype(jnp.bfloat16)
    hot = lax.broadcasted_iota(jnp.int32, (LANES, walls), 0) == jnp.broadcast_to(z, (LANES, walls))
    hot = jnp.where(hot, 1.0, 0.0).astype(jnp.bfloat16)
    dense = lax.dot_general(left, hot, (((1,), (1,)), ((), ())), preferred_element_type=jnp.float32)
    for x in range(size_x):
        low = dense[x * ROWS : (x + 1) * ROWS].astype(jnp.int32)
        high = dense[height + x * ROWS : height + (x + 1) * ROWS].astype(jnp.int32)
        state_o[REF, x] = ((high // 4) * LANES + low - 1).astype(jnp.float32)
        state_o[AXIS, x] = (high % 4).astype(jnp.float32)
    base = up(3 * (slots // LANES))
    parity = lax.axis_index(gy) % 2
    faces = []
    for b, y in ((2, ROWS - 1), (0, 0)):
        planes = [direction(a, b, c) for a in range(3) for c in range(3)] + list(range(RHO, PLANES))
        faces.append([state_o[plane, x, y : y + 1, :] for plane in planes for x in range(size_x)])
    for n, (above, below) in enumerate(zip(*faces)):
        even_o[base + n : base + n + 1, :] = jnp.where(parity == 0, above, below)
        odd_o[base + n : base + n + 1, :] = jnp.where(parity == 0, below, above)


def second_kernel(own, y_even, y_odd, *rest, gy, peers, slots, slots_each):
    state, rest = rest[0], rest[1:]
    far, outs = rest[: peers - 3], rest[peers - 3 :]
    post_o, edge_o, plus_o, minus_o = outs
    size_x = post_o.shape[1]
    width = slots // LANES
    base = up(3 * width)
    me = lax.axis_index(gy)
    below, above = (me + peers - 1) % peers, (me + 1) % peers
    y_parity = me % 2
    tables = [(own, me)]
    tables.append((y_even, jnp.where(y_parity == 0, above, below)))
    tables.append((y_odd, jnp.where(y_parity == 0, below, above)))
    for n, table in enumerate(far):
        tables.append((table, (me + peers - (n + 2)) % peers))

    def walled(block, ref, axis, vel):
        index = jnp.maximum(ref, 0)
        source = index // slots_each
        start = block * slots_each
        tile = start // LANES
        lane = start % LANES + index % slots_each
        out = []
        for d in range(3):
            picked = jnp.zeros(ref.shape, jnp.float32)
            for table, who in tables:
                row = table[pl.ds(d * width + tile, 1), :]
                got = lanes_of(jnp.broadcast_to(row, (ROWS, LANES)), lane)
                picked = jnp.where(source == who, got, picked)
            tangential = jnp.where(axis == d, 0.0, wall_ratio * picked)
            out.append(jnp.where(ref >= 0, tangential, vel[d]))
        return out

    plus, minus, corner_plus, corner_minus = [], [], [], []
    for x in range(size_x):
        ref = state[REF, x].astype(jnp.int32)
        axis = state[AXIS, x].astype(jnp.int32)
        vel = walled(me, ref, axis, [state[VEL + d, x] for d in range(3)])
        eq = equilibria(state[RHO, x], vel, range(27))
        for i in range(27):
            value = state[i, x] + eq[i]
            post_o[i, x] = value
            if x == size_x - 1 and i >= 18:
                plus.append(value)
            if x == 0 and i < 9:
                minus.append(value)
    plus.append(state[SOLID, size_x - 1])
    minus.append(state[SOLID, 0])
    sub = lax.broadcasted_iota(jnp.int32, (ROWS, LANES), 0)
    for side, (b, block) in enumerate(((2, below), (0, above))):

        def line(r):
            got = (y_odd[r : r + 1, :], y_even[r : r + 1, :])
            return jnp.where(y_parity == 0, got[side], got[1 - side])

        def plane(n):
            rows = [line(base + n * size_x + x) for x in range(size_x)]
            tile = jnp.broadcast_to(rows[0], (ROWS, LANES))
            for x in range(1, size_x):
                tile = jnp.where(sub == x, jnp.broadcast_to(rows[x], (ROWS, LANES)), tile)
            return tile

        ref = plane(13).astype(jnp.int32)
        axis = plane(14).astype(jnp.int32)
        vel = walled(block, ref, axis, [plane(10 + d) for d in range(3)])
        wanted = [direction(a, b, c) for a in range(3) for c in range(3)]
        eq = equilibria(plane(9), vel, wanted)
        for n, i in enumerate(wanted):
            value = plane(n) + eq[i]
            r = (side * 10 + n) * size_x
            edge_o[r : r + size_x, :] = value[:size_x]
            if i >= 18:
                corner_plus.append(value[size_x - 1 : size_x])
            if i < 9:
                corner_minus.append(value[0:1])
        solid = plane(15)
        r = (side * 10 + 9) * size_x
        edge_o[r : r + size_x, :] = solid[:size_x]
        corner_plus.append(solid[size_x - 1 : size_x])
        corner_minus.append(solid[0:1])
    for n in range(10):
        plus_o[n] = plus[n]
        minus_o[n] = minus[n]
    for n in range(8):
        plus_o[10, n : n + 1, :] = corner_plus[n]
        minus_o[10, n : n + 1, :] = corner_minus[n]


def third_kernel(post, edge, state, below, above, out_h, out, sems):
    size_x = post.shape[1]
    sub = lax.broadcasted_iota(jnp.int32, (ROWS, LANES), 0)
    corners = {-1: below[10], size_x: above[10]}

    def shifted(tile, row, step_y):
        if step_y == 0:
            return tile
        rolled = pltpu.roll(tile, step_y % ROWS, 0)
        return jnp.where(sub == (0 if step_y > 0 else ROWS - 1), jnp.broadcast_to(row, (ROWS, LANES)), rolled)

    def source(x, step_y, n_face, n_edge, n_corner, inside):
        side = 0 if step_y > 0 else 1
        if 0 <= x < size_x:
            tile = inside(x)
            r = (side * 10 + n_edge) * size_x + x
            row = edge[r : r + 1, :] if step_y else None
        else:
            tile = below[n_face] if x < 0 else above[n_face]
            row = corners[x][side * 4 + n_corner : side * 4 + n_corner + 1] if step_y else None
        return shifted(tile, row, step_y)

    copies = []
    for a in range(3):
        for b in range(3):
            for x in range(size_x):
                from_x, step_y = x - (a - 1), b - 1
                wall = source(from_x, step_y, 9, 9, 3, lambda q: state[SOLID, q])
                for c in range(3):
                    i = direction(a, b, c)
                    moved = source(from_x, step_y, 3 * b + c, 3 * a + c, c, lambda q: post[i, q])
                    solid = wall
                    if c != 1:
                        moved = pltpu.roll(moved, (c - 1) % LANES, 1)
                        solid = pltpu.roll(wall, (c - 1) % LANES, 1)
                    out[i, x] = jnp.where(solid > 0.5, post[26 - i, x], moved)
        copy = pltpu.make_async_copy(out.at[pl.ds(9 * a, 9)], out_h.at[pl.ds(9 * a, 9)], sems.at[a])
        copy.start()
        copies.append(copy)
    for copy in copies:
        copy.wait()


def local(
    populations, relax, solid, wall_cell, wall_normal, wall_count, sample_ref, stencil_cell, stencil_weight
):
    _, size_x, size_y, size_z = populations.shape
    walls, slots = wall_cell.shape[-1], stencil_cell.shape[-1]
    devices, peers = lax.axis_size("gx"), lax.axis_size("gy")
    slots_each = slots // peers
    if (size_y, size_z) != (ROWS, LANES) or walls % LANES or slots % LANES:
        raise ValueError("unsupported block")
    if LANES % slots_each or peers % 2 or peers < 4:
        raise ValueError("unsupported mesh")
    f32 = jnp.float32
    lines = up(3 * (slots // LANES))
    face = (lines + FACE * size_x, LANES)
    block = (size_x, ROWS, LANES)
    y_even, y_odd, samples, state = pl.pallas_call(
        lambda *refs: first_kernel(*refs, gy="gy"),
        out_shape=[
            jax.ShapeDtypeStruct(face, f32),
            jax.ShapeDtypeStruct(face, f32),
            jax.ShapeDtypeStruct((lines, LANES), f32),
            jax.ShapeDtypeStruct((PLANES, *block), f32),
        ],
        in_specs=[HBM] * 9,
        out_specs=[VMEM] * 4,
        scratch_shapes=[
            pltpu.VMEM(populations.shape, f32),
            pltpu.SMEM(relax.shape, f32),
            pltpu.VMEM(block, jnp.int32),
            pltpu.VMEM((1, walls), jnp.int32),
            pltpu.VMEM((1, walls), jnp.int32),
            pltpu.SMEM((1, 1), jnp.int32),
            pltpu.VMEM((1, walls), jnp.int32),
            pltpu.VMEM((8, slots), jnp.int32),
            pltpu.VMEM((8, slots), f32),
            pltpu.SemaphoreType.DMA((9,)),
        ],
        compiler_params=pltpu.CompilerParams(vmem_limit_bytes=GRANT),
        name="first",
    )(
        *(
            v if v is wall_count else pltpu.with_memory_space_constraint(v, pltpu.HBM)
            for v in (
                populations, relax, solid, wall_cell, wall_normal, wall_count, sample_ref, stencil_cell, stencil_weight
            )
        )
    )

    def swap(value, odd):
        return lax.ppermute(value, "gy", [(i, (((i - odd) ^ 1) + odd) % peers) for i in range(peers)])

    got_far = []
    for n in range(2, peers - 1):
        got_far.append(lax.ppermute(samples, "gy", [(i, (i + n) % peers) for i in range(peers)]))
    y_odd = swap(y_odd, 1)
    y_even = swap(y_even, 0)
    post, edge, plus, minus = pl.pallas_call(
        lambda *refs: second_kernel(*refs, gy="gy", peers=peers, slots=slots, slots_each=slots_each),
        out_shape=[
            jax.ShapeDtypeStruct(populations.shape, f32),
            jax.ShapeDtypeStruct((up(20 * size_x), LANES), f32),
            jax.ShapeDtypeStruct((11, ROWS, LANES), f32),
            jax.ShapeDtypeStruct((11, ROWS, LANES), f32),
        ],
        in_specs=[VMEM] * (4 + len(got_far)),
        out_specs=[VMEM] * 4,
        compiler_params=pltpu.CompilerParams(vmem_limit_bytes=GRANT),
        name="second",
    )(samples, y_even, y_odd, state, *got_far)
    from_below = lax.ppermute(plus, "gx", [(i, (i + 1) % devices) for i in range(devices)])
    from_above = lax.ppermute(minus, "gx", [(i, (i - 1) % devices) for i in range(devices)])
    return pl.pallas_call(
        third_kernel,
        out_shape=jax.ShapeDtypeStruct(populations.shape, f32),
        in_specs=[VMEM] * 5,
        out_specs=HBM,
        scratch_shapes=[pltpu.VMEM(populations.shape, f32), pltpu.SemaphoreType.DMA((3,))],
        compiler_params=pltpu.CompilerParams(vmem_limit_bytes=GRANT),
        name="third",
    )(post, edge, state, from_below, from_above)


def solution(mesh):
    return jax.shard_map(
        local,
        mesh=mesh,
        in_specs=(
            P(None, "gx", "gy", None),
            P(),
            P("gx", "gy", None),
            P("gx", "gy", None),
            P("gx", "gy", None),
            P("gx", "gy"),
            P("gx", "gy", None),
            P("gx", "gy", None, None),
            P("gx", "gy", None, None),
        ),
        out_specs=P(None, "gx", "gy", None),
        check_vma=False,
    )
```

```python
import jax
import jax.numpy as jnp
from jax import lax
from jax.experimental import pallas as pl
from jax.experimental.pallas import tpu as pltpu
from jax.sharding import PartitionSpec as P


wall_ratio = (1.0 / 9.0) ** (1.0 / 7.0)
LANES = 128
ROWS = 8
RHO, VEL, PLANES = 27, 28, 31
REF, AXIS, SOLID = 0, 1, 2
FACE = 16
HBM = pl.BlockSpec(memory_space=pltpu.HBM)
VMEM = pl.BlockSpec(memory_space=pltpu.VMEM)
COVER = 4 * 10**9
GRANT = 4 * 1024 * 1024


def direction(a, b, c):
    return 9 * a + 3 * b + c


def up(n):
    return -(-n // ROWS) * ROWS


def equilibria(density, velocity, wanted):
    ux, uy, uz = velocity
    rest = density * (1.0 - 1.5 * (ux * ux + uy * uy + uz * uz))
    out = {}
    for i in wanted:
        if i in out:
            continue
        step = (i // 9 - 1, i // 3 % 3 - 1, i % 3 - 1)
        along = None
        for s, u in zip(step, (ux, uy, uz)):
            if s:
                along = (u if s > 0 else -u) if along is None else (along + u if s > 0 else along - u)
        if along is None:
            out[i] = rest
            continue
        linear = density * along
        square = rest + 4.5 * (linear * along)
        out[i] = square + 3.0 * linear
        if 26 - i in wanted:
            out[26 - i] = square - 3.0 * linear
    return out


def along_axes(values, triple):
    for stride in (1, 3, 9):
        fresh = list(values)
        for i in range(27):
            if i // stride % 3 == 0:
                fresh[i], fresh[i + stride], fresh[i + 2 * stride] = triple(
                    values[i], values[i + stride], values[i + 2 * stride]
                )
        values = fresh
    return values


def relaxed(pops, keep):
    single = (1.0 / 6.0, 2.0 / 3.0, 1.0 / 6.0)
    weight = [single[i // 9] * single[i // 3 % 3] * single[i % 3] for i in range(27)]

    def raw(m, z, p):
        s = m + p
        return s + z, p - m, s

    def undo(m0, m1, m2):
        return m2 - m1, m0 - m2, m1 + m2

    moment = along_axes([w * p for w, p in zip(weight, pops)], raw)
    density = moment[0]
    inv = 1.0 / density
    vel = [moment[9] * inv, moment[3] * inv, moment[1] * inv]
    first = [moment[9], moment[3], moment[1]]
    second = [4.5 * (j * u) for j, u in zip(first, vel)]
    rest = density - (1.0 / 3.0) * (second[0] + second[1] + second[2])
    mu, nu, ka = (1.0, 0.0, 1.0 / 3.0), (0.0, 1.0 / 3.0, 0.0), (1.0 / 3.0, 0.0, 1.0 / 3.0)
    cross = {}
    kept = []
    for i in range(27):
        p = (i // 9, i // 3 % 3, i % 3)
        eq = None
        terms = [(mu[p[0]] * mu[p[1]] * mu[p[2]], rest)]
        for d in range(3):
            o, q = [e for e in range(3) if e != d]
            terms.append((3.0 * nu[p[d]] * mu[p[o]] * mu[p[q]], first[d]))
            terms.append((ka[p[d]] * mu[p[o]] * mu[p[q]], second[d]))
            factor = 9.0 * nu[p[o]] * nu[p[q]] * mu[p[d]]
            if factor:
                if d not in cross:
                    cross[d] = first[o] * vel[q]
                terms.append((factor, cross[d]))
        for f, t in terms:
            if f:
                t = t if abs(f - 1.0) < 1e-12 else f * t
                eq = t if eq is None else eq + t
        dev = moment[i] if eq is None else moment[i] - eq
        kept.append(keep[i] * dev)
    back = (3.0, 1.5, 3.0)
    kept = along_axes(kept, undo)
    kept = [back[i // 9] * back[i // 3 % 3] * back[i % 3] * k for i, k in enumerate(kept)]
    return density, vel, kept


def lanes_of(table, index):
    return jnp.take_along_axis(table, index, axis=1, mode="promise_in_bounds")


def number_kernel(out):
    out[...] = lax.broadcasted_iota(jnp.int32, out.shape, 1)


def live_kernel(number, cell, normal, ref, relax, count, cell_o, axis_o, ref_o, keep_o):
    cell_o[...] = jnp.where(number[...] < count[0, 0], cell[0], -1)
    axis_o[...] = normal[0] // 2
    ref_o[...] = ref[0]
    keep_o[...] = 1.0 - relax[...]


def cell_kernel(keep, pop, scell, sweight, state_o, sample_o):
    size_x, slots = pop.shape[1], scell.shape[-1]
    rates = [jnp.broadcast_to(keep[0:1, i : i + 1], (ROWS, LANES)) for i in range(27)]
    velocity = []
    for x in range(size_x):
        density, vel, kept = relaxed([pop[i, x] for i in range(27)], rates)
        velocity.append(vel)
        for i in range(27):
            state_o[i, x] = kept[i]
        state_o[RHO, x] = density
        for d in range(3):
            state_o[VEL + d, x] = vel[d]
    sub = lax.broadcasted_iota(jnp.int32, (ROWS, LANES), 0)
    for t in range(slots // LANES):
        cells = scell[0, 0, :, t * LANES : (t + 1) * LANES]
        weights = sweight[0, 0, :, t * LANES : (t + 1) * LANES]
        row, z = cells // LANES, cells % LANES
        low = jnp.broadcast_to(z[0:1], (ROWS, LANES))
        other = z != low
        high = jnp.max(jnp.where(other, z, 0), axis=0, keepdims=True)
        high = jnp.broadcast_to(high, (ROWS, LANES))
        w_high = jnp.where(other, weights, 0.0)
        w_low = weights - w_high
        total = [None] * 3
        for x in range(size_x):
            a_low = jnp.zeros((ROWS, LANES), jnp.float32)
            a_high = a_low
            for k in range(8):
                hit = jnp.broadcast_to(row[k : k + 1], (ROWS, LANES)) == sub + x * ROWS
                a_low += jnp.where(hit, jnp.broadcast_to(w_low[k : k + 1], (ROWS, LANES)), 0.0)
                a_high += jnp.where(hit, jnp.broadcast_to(w_high[k : k + 1], (ROWS, LANES)), 0.0)
            for d in range(3):
                part = a_low * lanes_of(velocity[x][d], low) + a_high * lanes_of(velocity[x][d], high)
                total[d] = part if total[d] is None else total[d] + part
        for d in range(3):
            r = d * (slots // LANES) + t
            sample_o[r : r + 1, :] = jnp.sum(total[d], axis=0, keepdims=True)


def face_kernel(cell, axis, ref, solid, state, sample, even_o, odd_o, early_o, map_o, *, gy):
    size_x, walls = solid.shape[0], cell.shape[-1]
    row = jnp.where(cell[...] < 0, -1, cell[...] // LANES)
    z = cell[...] % LANES
    low = (ref[...] % LANES + 1).astype(jnp.float32)
    high = (ref[...] // LANES * 4 + axis[...]).astype(jnp.float32)
    height = size_x * ROWS
    at = lax.broadcasted_iota(jnp.int32, (height, walls), 0) == jnp.broadcast_to(row, (height, walls))
    left = jnp.concatenate(
        [jnp.where(at, jnp.broadcast_to(v, (height, walls)), 0.0) for v in (low, high)], axis=0
    ).astype(jnp.bfloat16)
    hot = lax.broadcasted_iota(jnp.int32, (LANES, walls), 0) == jnp.broadcast_to(z, (LANES, walls))
    hot = jnp.where(hot, 1.0, 0.0).astype(jnp.bfloat16)
    dense = lax.dot_general(left, hot, (((1,), (1,)), ((), ())), preferred_element_type=jnp.float32)
    for x in range(size_x):
        low = dense[x * ROWS : (x + 1) * ROWS].astype(jnp.int32)
        high = dense[height + x * ROWS : height + (x + 1) * ROWS].astype(jnp.int32)
        map_o[REF, x] = ((high // 4) * LANES + low - 1).astype(jnp.float32)
        map_o[AXIS, x] = (high % 4).astype(jnp.float32)
        map_o[SOLID, x] = solid[x].astype(jnp.float32)
    for n in range(9):
        early_o[n] = state[18 + n, size_x - 1]
    early_o[9] = state[RHO, size_x - 1]
    early_o[10] = map_o[SOLID, size_x - 1]
    base = sample.shape[0]
    even_o[:base, :] = sample[...]
    odd_o[:base, :] = sample[...]
    parity = lax.axis_index(gy) % 2
    faces = []
    for b, y in ((2, ROWS - 1), (0, 0)):
        planes = [(state, direction(a, b, c)) for a in range(3) for c in range(3)]
        planes += [(state, n) for n in range(RHO, PLANES)] + [(map_o, n) for n in range(3)]
        faces.append([array[plane, x, y : y + 1, :] for array, plane in planes for x in range(size_x)])
    for n, (above, below) in enumerate(zip(*faces)):
        even_o[base + n : base + n + 1, :] = jnp.where(parity == 0, above, below)
        odd_o[base + n : base + n + 1, :] = jnp.where(parity == 0, below, above)


def second_kernel(own, y_even, y_odd, *rest, gy, peers, slots, slots_each):
    state, maps, rest = rest[0], rest[1], rest[2:]
    far, outs = rest[: peers - 3], rest[peers - 3 :]
    post_o, edge_o, plus_o, minus_o = outs
    size_x = post_o.shape[1]
    width = slots // LANES
    base = up(3 * width)
    me = lax.axis_index(gy)
    below, above = (me + peers - 1) % peers, (me + 1) % peers
    y_parity = me % 2
    tables = [(own, me)]
    tables.append((y_even, jnp.where(y_parity == 0, above, below)))
    tables.append((y_odd, jnp.where(y_parity == 0, below, above)))
    for n, table in enumerate(far):
        tables.append((table, (me + peers - (n + 2)) % peers))

    def walled(block, ref, axis, vel):
        index = jnp.maximum(ref, 0)
        source = index // slots_each
        start = block * slots_each
        tile = start // LANES
        lane = start % LANES + index % slots_each
        out = []
        for d in range(3):
            picked = jnp.zeros(ref.shape, jnp.float32)
            for table, who in tables:
                row = table[pl.ds(d * width + tile, 1), :]
                got = lanes_of(jnp.broadcast_to(row, (ROWS, LANES)), lane)
                picked = jnp.where(source == who, got, picked)
            tangential = jnp.where(axis == d, 0.0, wall_ratio * picked)
            out.append(jnp.where(ref >= 0, tangential, vel[d]))
        return out

    minus, corner_plus, corner_minus = [], [], []
    for x in range(size_x):
        ref = maps[REF, x].astype(jnp.int32)
        axis = maps[AXIS, x].astype(jnp.int32)
        vel = walled(me, ref, axis, [state[VEL + d, x] for d in range(3)])
        if x == size_x - 1:
            for d in range(3):
                plus_o[d] = vel[d]
        eq = equilibria(state[RHO, x], vel, range(27))
        for i in range(27):
            value = state[i, x] + eq[i]
            post_o[i, x] = value
            if x == 0 and i < 9:
                minus.append(value)
    minus.append(maps[SOLID, 0])
    sub = lax.broadcasted_iota(jnp.int32, (ROWS, LANES), 0)
    for side, (b, block) in enumerate(((2, below), (0, above))):

        def line(r):
            got = (y_odd[r : r + 1, :], y_even[r : r + 1, :])
            return jnp.where(y_parity == 0, got[side], got[1 - side])

        def plane(n):
            rows = [line(base + n * size_x + x) for x in range(size_x)]
            tile = jnp.broadcast_to(rows[0], (ROWS, LANES))
            for x in range(1, size_x):
                tile = jnp.where(sub == x, jnp.broadcast_to(rows[x], (ROWS, LANES)), tile)
            return tile

        ref = plane(13).astype(jnp.int32)
        axis = plane(14).astype(jnp.int32)
        vel = walled(block, ref, axis, [plane(10 + d) for d in range(3)])
        wanted = [direction(a, b, c) for a in range(3) for c in range(3)]
        eq = equilibria(plane(9), vel, wanted)
        for n, i in enumerate(wanted):
            value = plane(n) + eq[i]
            r = (side * 10 + n) * size_x
            edge_o[r : r + size_x, :] = value[:size_x]
            if i >= 18:
                corner_plus.append(value[size_x - 1 : size_x])
            if i < 9:
                corner_minus.append(value[0:1])
        solid = plane(15)
        r = (side * 10 + 9) * size_x
        edge_o[r : r + size_x, :] = solid[:size_x]
        corner_plus.append(solid[size_x - 1 : size_x])
        corner_minus.append(solid[0:1])
    for n in range(10):
        minus_o[n] = minus[n]
    for n in range(8):
        plus_o[3, n : n + 1, :] = corner_plus[n]
        minus_o[10, n : n + 1, :] = corner_minus[n]


def shifted(tile, row, step_y):
    if step_y == 0:
        return tile
    sub = lax.broadcasted_iota(jnp.int32, (ROWS, LANES), 0)
    rolled = pltpu.roll(tile, step_y % ROWS, 0)
    return jnp.where(sub == (0 if step_y > 0 else ROWS - 1), jnp.broadcast_to(row, (ROWS, LANES)), rolled)


def along_z(tile, c):
    return tile if c == 1 else pltpu.roll(tile, (c - 1) % LANES, 1)


def inner_kernel(post, edge, maps, out_h, out, sems):
    size_x = post.shape[1]
    copies = []
    for a in (1, 2, 0):
        first, last = max(a - 1, 0), size_x + min(a - 1, 0)
        for b in range(3):
            side = 0 if b == 2 else 1
            for x in range(first, last):
                q = x - (a - 1)

                def row(n):
                    r = (side * 10 + n) * size_x + q
                    return edge[r : r + 1, :]

                wall = shifted(maps[SOLID, q], row(9), b - 1)
                for c in range(3):
                    i = direction(a, b, c)
                    moved = along_z(shifted(post[i, q], row(3 * a + c), b - 1), c)
                    out[i, x] = jnp.where(along_z(wall, c) > 0.5, post[26 - i, x], moved)
        part = (pl.ds(9 * a, 9), pl.ds(first, last - first))
        copy = pltpu.make_async_copy(out.at[part], out_h.at[part], sems.at[a])
        copy.start()
        copies.append(copy)
    for copy in copies:
        copy.wait()


def outer_kernel(post, early, below, above, held_h, out_h, out, sems):
    del held_h
    size_x = post.shape[1]
    copies = []
    for a, x in ((0, size_x - 1), (2, 0)):
        if a == 0:
            tiles, solid, corner = [above[n] for n in range(9)], above[9], above[10]
        else:
            eq = equilibria(early[9], [below[d] for d in range(3)], range(18, 27))
            tiles, solid, corner = [early[n] + eq[18 + n] for n in range(9)], early[10], below[3]
        for b in range(3):
            side = 0 if b == 2 else 1
            wall = shifted(solid, corner[side * 4 + 3 : side * 4 + 4], b - 1)
            for c in range(3):
                i = direction(a, b, c)
                moved = shifted(tiles[3 * b + c], corner[side * 4 + c : side * 4 + c + 1], b - 1)
                moved = along_z(moved, c)
                out[i % 9 + 9 * (a // 2)] = jnp.where(along_z(wall, c) > 0.5, post[26 - i, x], moved)
        copy = pltpu.make_async_copy(out.at[pl.ds(9 * (a // 2), 9)], out_h.at[pl.ds(9 * a, 9), x], sems.at[a // 2])
        copy.start()
        copies.append(copy)
    for copy in copies:
        copy.wait()


def local(
    populations, relax, solid, wall_cell, wall_normal, wall_count, sample_ref, stencil_cell, stencil_weight
):
    _, size_x, size_y, size_z = populations.shape
    walls, slots = wall_cell.shape[-1], stencil_cell.shape[-1]
    devices, peers = lax.axis_size("gx"), lax.axis_size("gy")
    slots_each = slots // peers
    if (size_y, size_z) != (ROWS, LANES) or walls % LANES or slots % LANES:
        raise ValueError("unsupported block")
    if LANES % slots_each or peers % 2 or peers < 4:
        raise ValueError("unsupported mesh")
    f32 = jnp.float32
    lines = up(3 * (slots // LANES))
    face = (lines + FACE * size_x, LANES)
    block = (size_x, ROWS, LANES)
    number = pl.pallas_call(
        number_kernel,
        out_shape=jax.ShapeDtypeStruct((1, walls), jnp.int32),
        out_specs=VMEM,
        cost_estimate=pl.CostEstimate(flops=COVER, bytes_accessed=0, transcendentals=0),
        compiler_params=pltpu.CompilerParams(vmem_limit_bytes=GRANT),
        name="number",
    )()
    wall_row = jax.ShapeDtypeStruct((1, walls), jnp.int32)
    cells, axis, refs, keep = pl.pallas_call(
        live_kernel,
        out_shape=[wall_row, wall_row, wall_row, jax.ShapeDtypeStruct((1, 27), f32)],
        in_specs=[VMEM] * 5 + [pl.BlockSpec(memory_space=pltpu.SMEM)],
        out_specs=[VMEM] * 4,
        compiler_params=pltpu.CompilerParams(vmem_limit_bytes=GRANT),
        name="live",
    )(number, wall_cell, wall_normal, sample_ref, relax.reshape(1, 27), wall_count)
    state, samples = pl.pallas_call(
        cell_kernel,
        out_shape=[jax.ShapeDtypeStruct((PLANES, *block), f32), jax.ShapeDtypeStruct((lines, LANES), f32)],
        in_specs=[VMEM] * 4,
        out_specs=[VMEM] * 2,
        compiler_params=pltpu.CompilerParams(vmem_limit_bytes=GRANT),
        name="cells",
    )(keep, populations, stencil_cell, stencil_weight)
    y_even, y_odd, early, maps = pl.pallas_call(
        lambda *refs: face_kernel(*refs, gy="gy"),
        out_shape=[
            jax.ShapeDtypeStruct(face, f32),
            jax.ShapeDtypeStruct(face, f32),
            jax.ShapeDtypeStruct((11, ROWS, LANES), f32),
            jax.ShapeDtypeStruct((3, *block), f32),
        ],
        in_specs=[VMEM] * 6,
        out_specs=[VMEM] * 4,
        compiler_params=pltpu.CompilerParams(vmem_limit_bytes=GRANT),
        name="face",
    )(cells, axis, refs, solid, state, samples)

    def swap(value, odd):
        return lax.ppermute(value, "gy", [(i, (((i - odd) ^ 1) + odd) % peers) for i in range(peers)])

    got_far = []
    for n in range(2, peers - 1):
        got_far.append(lax.ppermute(samples, "gy", [(i, (i + n) % peers) for i in range(peers)]))
    y_odd = swap(y_odd, 1)
    y_even = swap(y_even, 0)
    ring = [(i, (i + 1) % devices) for i in range(devices)]
    early = lax.ppermute(early, "gx", ring)
    post, edge, plus, minus = pl.pallas_call(
        lambda *refs: second_kernel(*refs, gy="gy", peers=peers, slots=slots, slots_each=slots_each),
        out_shape=[
            jax.ShapeDtypeStruct(populations.shape, f32),
            jax.ShapeDtypeStruct((up(20 * size_x), LANES), f32),
            jax.ShapeDtypeStruct((4, ROWS, LANES), f32),
            jax.ShapeDtypeStruct((11, ROWS, LANES), f32),
        ],
        in_specs=[VMEM] * (5 + len(got_far)),
        out_specs=[VMEM] * 4,
        compiler_params=pltpu.CompilerParams(vmem_limit_bytes=GRANT),
        name="second",
    )(samples, y_even, y_odd, state, maps, *got_far)
    from_below = lax.ppermute(plus, "gx", ring)
    from_above = lax.ppermute(minus, "gx", [(i, (i - 1) % devices) for i in range(devices)])
    held = pl.pallas_call(
        inner_kernel,
        out_shape=jax.ShapeDtypeStruct(populations.shape, f32),
        in_specs=[VMEM] * 3,
        out_specs=HBM,
        scratch_shapes=[pltpu.VMEM(populations.shape, f32), pltpu.SemaphoreType.DMA((3,))],
        compiler_params=pltpu.CompilerParams(vmem_limit_bytes=GRANT),
        name="inner",
    )(post, edge, maps)
    return pl.pallas_call(
        outer_kernel,
        out_shape=jax.ShapeDtypeStruct(populations.shape, f32),
        in_specs=[VMEM] * 4 + [HBM],
        out_specs=HBM,
        input_output_aliases={4: 0},
        scratch_shapes=[pltpu.VMEM((18, ROWS, LANES), f32), pltpu.SemaphoreType.DMA((2,))],
        compiler_params=pltpu.CompilerParams(vmem_limit_bytes=GRANT),
        name="outer",
    )(post, early, from_below, from_above, pltpu.with_memory_space_constraint(held, pltpu.HBM))


def solution(mesh):
    return jax.shard_map(
        local,
        mesh=mesh,
        in_specs=(
            P(None, "gx", "gy", None),
            P(),
            P("gx", "gy", None),
            P("gx", "gy", None),
            P("gx", "gy", None),
            P("gx", "gy"),
            P("gx", "gy", None),
            P("gx", "gy", None, None),
            P("gx", "gy", None, None),
        ),
        out_specs=P(None, "gx", "gy", None),
        check_vma=False,
    )
```

```python
import jax
import jax.numpy as jnp
from jax import lax
from jax.experimental import pallas as pl
from jax.experimental.pallas import tpu as pltpu
from jax.sharding import PartitionSpec as P


wall_ratio = (1.0 / 9.0) ** (1.0 / 7.0)
LANES = 128
ROWS = 8
RHO, VEL, PLANES = 27, 28, 31
REF, AXIS, SOLID = 0, 1, 2
FACE = 16
HBM = pl.BlockSpec(memory_space=pltpu.HBM)
VMEM = pl.BlockSpec(memory_space=pltpu.VMEM)
THROUGH = ("normal", "ref", "relax")
COVER = 4 * 10**9
GRANT = 4 * 1024 * 1024


def direction(a, b, c):
    return 9 * a + 3 * b + c


def up(n):
    return -(-n // ROWS) * ROWS


def equilibria(density, velocity, wanted):
    ux, uy, uz = velocity
    rest = density * (1.0 - 1.5 * (ux * ux + uy * uy + uz * uz))
    out = {}
    for i in wanted:
        if i in out:
            continue
        step = (i // 9 - 1, i // 3 % 3 - 1, i % 3 - 1)
        along = None
        for s, u in zip(step, (ux, uy, uz)):
            if s:
                along = (u if s > 0 else -u) if along is None else (along + u if s > 0 else along - u)
        if along is None:
            out[i] = rest
            continue
        linear = density * along
        square = rest + 4.5 * (linear * along)
        out[i] = square + 3.0 * linear
        if 26 - i in wanted:
            out[26 - i] = square - 3.0 * linear
    return out


def along_axes(values, triple):
    for stride in (1, 3, 9):
        fresh = list(values)
        for i in range(27):
            if i // stride % 3 == 0:
                fresh[i], fresh[i + stride], fresh[i + 2 * stride] = triple(
                    values[i], values[i + stride], values[i + 2 * stride]
                )
        values = fresh
    return values


def relaxed(pops, keep):
    single = (1.0 / 6.0, 2.0 / 3.0, 1.0 / 6.0)
    weight = [single[i // 9] * single[i // 3 % 3] * single[i % 3] for i in range(27)]

    def raw(m, z, p):
        s = m + p
        return s + z, p - m, s

    def undo(m0, m1, m2):
        return m2 - m1, m0 - m2, m1 + m2

    moment = along_axes([w * p for w, p in zip(weight, pops)], raw)
    density = moment[0]
    inv = 1.0 / density
    vel = [moment[9] * inv, moment[3] * inv, moment[1] * inv]
    first = [moment[9], moment[3], moment[1]]
    second = [4.5 * (j * u) for j, u in zip(first, vel)]
    rest = density - (1.0 / 3.0) * (second[0] + second[1] + second[2])
    mu, nu, ka = (1.0, 0.0, 1.0 / 3.0), (0.0, 1.0 / 3.0, 0.0), (1.0 / 3.0, 0.0, 1.0 / 3.0)
    cross = {}
    kept = []
    for i in range(27):
        p = (i // 9, i // 3 % 3, i % 3)
        eq = None
        terms = [(mu[p[0]] * mu[p[1]] * mu[p[2]], rest)]
        for d in range(3):
            o, q = [e for e in range(3) if e != d]
            terms.append((3.0 * nu[p[d]] * mu[p[o]] * mu[p[q]], first[d]))
            terms.append((ka[p[d]] * mu[p[o]] * mu[p[q]], second[d]))
            factor = 9.0 * nu[p[o]] * nu[p[q]] * mu[p[d]]
            if factor:
                if d not in cross:
                    cross[d] = first[o] * vel[q]
                terms.append((factor, cross[d]))
        for f, t in terms:
            if f:
                t = t if abs(f - 1.0) < 1e-12 else f * t
                eq = t if eq is None else eq + t
        dev = moment[i] if eq is None else moment[i] - eq
        kept.append(keep[i] * dev)
    back = (3.0, 1.5, 3.0)
    kept = along_axes(kept, undo)
    kept = [back[i // 9] * back[i // 3 % 3] * back[i % 3] * k for i, k in enumerate(kept)]
    return density, vel, kept


def lanes_of(table, index):
    return jnp.take_along_axis(table, index, axis=1, mode="promise_in_bounds")


def number_kernel(out):
    out[...] = lax.broadcasted_iota(jnp.int32, out.shape, 1)


def live_kernel(number, count, cell, *rest):
    half = (len(rest) - 1) // 2
    rest[half][...] = jnp.where(number[...] < count[0, 0], cell[0], -1)
    for source, target in zip(rest[:half], rest[half + 1 :]):
        target[...] = source[...]


def cell_kernel(relax, pop, scell, sweight, state_o, sample_o):
    size_x, slots = pop.shape[1], scell.shape[-1]
    rates = [1.0 - jnp.broadcast_to(relax[0:1, i : i + 1], (ROWS, LANES)) for i in range(27)]
    velocity = []
    for x in range(size_x):
        density, vel, kept = relaxed([pop[i, x] for i in range(27)], rates)
        velocity.append(vel)
        for i in range(27):
            state_o[i, x] = kept[i]
        state_o[RHO, x] = density
        for d in range(3):
            state_o[VEL + d, x] = vel[d]
    sub = lax.broadcasted_iota(jnp.int32, (ROWS, LANES), 0)
    for t in range(slots // LANES):
        cells = scell[0, 0, :, t * LANES : (t + 1) * LANES]
        weights = sweight[0, 0, :, t * LANES : (t + 1) * LANES]
        row, z = cells // LANES, cells % LANES
        low = jnp.broadcast_to(z[0:1], (ROWS, LANES))
        other = z != low
        high = jnp.max(jnp.where(other, z, 0), axis=0, keepdims=True)
        high = jnp.broadcast_to(high, (ROWS, LANES))
        w_high = jnp.where(other, weights, 0.0)
        w_low = weights - w_high
        total = [None] * 3
        for x in range(size_x):
            a_low = jnp.zeros((ROWS, LANES), jnp.float32)
            a_high = a_low
            for k in range(8):
                hit = jnp.broadcast_to(row[k : k + 1], (ROWS, LANES)) == sub + x * ROWS
                a_low += jnp.where(hit, jnp.broadcast_to(w_low[k : k + 1], (ROWS, LANES)), 0.0)
                a_high += jnp.where(hit, jnp.broadcast_to(w_high[k : k + 1], (ROWS, LANES)), 0.0)
            for d in range(3):
                part = a_low * lanes_of(velocity[x][d], low) + a_high * lanes_of(velocity[x][d], high)
                total[d] = part if total[d] is None else total[d] + part
        for d in range(3):
            r = d * (slots // LANES) + t
            sample_o[r : r + 1, :] = jnp.sum(total[d], axis=0, keepdims=True)


def face_kernel(cell, normal, ref, solid, state, sample, even_o, odd_o, early_o, map_o, *, gy):
    size_x, walls = solid.shape[0], cell.shape[-1]
    row = jnp.where(cell[...] < 0, -1, cell[...] // LANES)
    z = cell[...] % LANES
    low = (ref[0] % LANES + 1).astype(jnp.float32)
    high = (ref[0] // LANES * 4 + normal[0] // 2).astype(jnp.float32)
    height = size_x * ROWS
    at = lax.broadcasted_iota(jnp.int32, (height, walls), 0) == jnp.broadcast_to(row, (height, walls))
    left = jnp.concatenate(
        [jnp.where(at, jnp.broadcast_to(v, (height, walls)), 0.0) for v in (low, high)], axis=0
    ).astype(jnp.bfloat16)
    hot = lax.broadcasted_iota(jnp.int32, (LANES, walls), 0) == jnp.broadcast_to(z, (LANES, walls))
    hot = jnp.where(hot, 1.0, 0.0).astype(jnp.bfloat16)
    dense = lax.dot_general(left, hot, (((1,), (1,)), ((), ())), preferred_element_type=jnp.float32)
    for x in range(size_x):
        low = dense[x * ROWS : (x + 1) * ROWS].astype(jnp.int32)
        high = dense[height + x * ROWS : height + (x + 1) * ROWS].astype(jnp.int32)
        map_o[REF, x] = ((high // 4) * LANES + low - 1).astype(jnp.float32)
        map_o[AXIS, x] = (high % 4).astype(jnp.float32)
        map_o[SOLID, x] = solid[x].astype(jnp.float32)
    for n in range(9):
        early_o[n] = state[18 + n, size_x - 1]
    early_o[9] = state[RHO, size_x - 1]
    early_o[10] = map_o[SOLID, size_x - 1]
    base = sample.shape[0]
    even_o[:base, :] = sample[...]
    odd_o[:base, :] = sample[...]
    parity = lax.axis_index(gy) % 2
    faces = []
    for b, y in ((2, ROWS - 1), (0, 0)):
        planes = [(state, direction(a, b, c)) for a in range(3) for c in range(3)]
        planes += [(state, n) for n in range(RHO, PLANES)] + [(map_o, n) for n in range(3)]
        faces.append([array[plane, x, y : y + 1, :] for array, plane in planes for x in range(size_x)])
    for n, (above, below) in enumerate(zip(*faces)):
        even_o[base + n : base + n + 1, :] = jnp.where(parity == 0, above, below)
        odd_o[base + n : base + n + 1, :] = jnp.where(parity == 0, below, above)


def first_kernel(
    cells, normal, ref, relax, solid, scell, sweight, pop, even_o, odd_o, sample_o, state_o, early_o, map_o, *, gy
):
    cell_kernel(relax, pop, scell, sweight, state_o, sample_o)
    face_kernel(cells, normal, ref, solid, state_o, sample_o, even_o, odd_o, early_o, map_o, gy=gy)


def second_kernel(own, y_even, y_odd, *rest, gy, peers, slots, slots_each):
    state, maps, rest = rest[0], rest[1], rest[2:]
    far, outs = rest[: peers - 3], rest[peers - 3 :]
    post_o, edge_o, plus_o, minus_o = outs
    size_x = post_o.shape[1]
    width = slots // LANES
    base = up(3 * width)
    me = lax.axis_index(gy)
    below, above = (me + peers - 1) % peers, (me + 1) % peers
    y_parity = me % 2
    tables = [(own, me)]
    tables.append((y_even, jnp.where(y_parity == 0, above, below)))
    tables.append((y_odd, jnp.where(y_parity == 0, below, above)))
    for n, table in enumerate(far):
        tables.append((table, (me + peers - (n + 2)) % peers))

    def walled(block, ref, axis, vel):
        index = jnp.maximum(ref, 0)
        source = index // slots_each
        start = block * slots_each
        tile = start // LANES
        lane = start % LANES + index % slots_each
        out = []
        for d in range(3):
            picked = jnp.zeros(ref.shape, jnp.float32)
            for table, who in tables:
                row = table[pl.ds(d * width + tile, 1), :]
                got = lanes_of(jnp.broadcast_to(row, (ROWS, LANES)), lane)
                picked = jnp.where(source == who, got, picked)
            tangential = jnp.where(axis == d, 0.0, wall_ratio * picked)
            out.append(jnp.where(ref >= 0, tangential, vel[d]))
        return out

    minus, corner_plus, corner_minus = [], [], []
    for x in range(size_x):
        ref = maps[REF, x].astype(jnp.int32)
        axis = maps[AXIS, x].astype(jnp.int32)
        vel = walled(me, ref, axis, [state[VEL + d, x] for d in range(3)])
        if x == size_x - 1:
            for d in range(3):
                plus_o[d] = vel[d]
        eq = equilibria(state[RHO, x], vel, range(27))
        for i in range(27):
            value = state[i, x] + eq[i]
            post_o[i, x] = value
            if x == 0 and i < 9:
                minus.append(value)
    minus.append(maps[SOLID, 0])
    sub = lax.broadcasted_iota(jnp.int32, (ROWS, LANES), 0)
    for side, (b, block) in enumerate(((2, below), (0, above))):

        def line(r):
            got = (y_odd[r : r + 1, :], y_even[r : r + 1, :])
            return jnp.where(y_parity == 0, got[side], got[1 - side])

        def plane(n):
            rows = [line(base + n * size_x + x) for x in range(size_x)]
            tile = jnp.broadcast_to(rows[0], (ROWS, LANES))
            for x in range(1, size_x):
                tile = jnp.where(sub == x, jnp.broadcast_to(rows[x], (ROWS, LANES)), tile)
            return tile

        ref = plane(13).astype(jnp.int32)
        axis = plane(14).astype(jnp.int32)
        vel = walled(block, ref, axis, [plane(10 + d) for d in range(3)])
        wanted = [direction(a, b, c) for a in range(3) for c in range(3)]
        eq = equilibria(plane(9), vel, wanted)
        for n, i in enumerate(wanted):
            value = plane(n) + eq[i]
            r = (side * 10 + n) * size_x
            edge_o[r : r + size_x, :] = value[:size_x]
            if i >= 18:
                corner_plus.append(value[size_x - 1 : size_x])
            if i < 9:
                corner_minus.append(value[0:1])
        solid = plane(15)
        r = (side * 10 + 9) * size_x
        edge_o[r : r + size_x, :] = solid[:size_x]
        corner_plus.append(solid[size_x - 1 : size_x])
        corner_minus.append(solid[0:1])
    for n in range(10):
        minus_o[n] = minus[n]
    for n in range(8):
        plus_o[3, n : n + 1, :] = corner_plus[n]
        minus_o[10, n : n + 1, :] = corner_minus[n]


def shifted(tile, row, step_y):
    if step_y == 0:
        return tile
    sub = lax.broadcasted_iota(jnp.int32, (ROWS, LANES), 0)
    rolled = pltpu.roll(tile, step_y % ROWS, 0)
    return jnp.where(sub == (0 if step_y > 0 else ROWS - 1), jnp.broadcast_to(row, (ROWS, LANES)), rolled)


def along_z(tile, c):
    return tile if c == 1 else pltpu.roll(tile, (c - 1) % LANES, 1)


def inner_kernel(post, edge, maps, out_h, out, sems):
    size_x = post.shape[1]
    copies = []
    for a in (1, 2, 0):
        first, last = max(a - 1, 0), size_x + min(a - 1, 0)
        for b in range(3):
            side = 0 if b == 2 else 1
            for x in range(first, last):
                q = x - (a - 1)

                def row(n):
                    r = (side * 10 + n) * size_x + q
                    return edge[r : r + 1, :]

                wall = shifted(maps[SOLID, q], row(9), b - 1)
                for c in range(3):
                    i = direction(a, b, c)
                    moved = along_z(shifted(post[i, q], row(3 * a + c), b - 1), c)
                    out[i, x] = jnp.where(along_z(wall, c) > 0.5, post[26 - i, x], moved)
        part = (pl.ds(9 * a, 9), pl.ds(first, last - first))
        copy = pltpu.make_async_copy(out.at[part], out_h.at[part], sems.at[a])
        copy.start()
        copies.append(copy)
    for copy in copies:
        copy.wait()


def outer_kernel(post, early, below, above, held_h, out_h, out, sems):
    del held_h
    size_x = post.shape[1]
    copies = []
    for a, x in ((0, size_x - 1), (2, 0)):
        if a == 0:
            tiles, solid, corner = [above[n] for n in range(9)], above[9], above[10]
        else:
            eq = equilibria(early[9], [below[d] for d in range(3)], range(18, 27))
            tiles, solid, corner = [early[n] + eq[18 + n] for n in range(9)], early[10], below[3]
        for b in range(3):
            side = 0 if b == 2 else 1
            wall = shifted(solid, corner[side * 4 + 3 : side * 4 + 4], b - 1)
            for c in range(3):
                i = direction(a, b, c)
                moved = shifted(tiles[3 * b + c], corner[side * 4 + c : side * 4 + c + 1], b - 1)
                moved = along_z(moved, c)
                out[i % 9 + 9 * (a // 2)] = jnp.where(along_z(wall, c) > 0.5, post[26 - i, x], moved)
        copy = pltpu.make_async_copy(out.at[pl.ds(9 * (a // 2), 9)], out_h.at[pl.ds(9 * a, 9), x], sems.at[a // 2])
        copy.start()
        copies.append(copy)
    for copy in copies:
        copy.wait()


def local(
    populations, relax, solid, wall_cell, wall_normal, wall_count, sample_ref, stencil_cell, stencil_weight
):
    _, size_x, size_y, size_z = populations.shape
    walls, slots = wall_cell.shape[-1], stencil_cell.shape[-1]
    devices, peers = lax.axis_size("gx"), lax.axis_size("gy")
    slots_each = slots // peers
    if (size_y, size_z) != (ROWS, LANES) or walls % LANES or slots % LANES:
        raise ValueError("unsupported block")
    if LANES % slots_each or peers % 2 or peers < 4:
        raise ValueError("unsupported mesh")
    f32 = jnp.float32
    lines = up(3 * (slots // LANES))
    face = (lines + FACE * size_x, LANES)
    block = (size_x, ROWS, LANES)
    number = pl.pallas_call(
        number_kernel,
        out_shape=jax.ShapeDtypeStruct((1, walls), jnp.int32),
        out_specs=VMEM,
        cost_estimate=pl.CostEstimate(flops=COVER, bytes_accessed=0, transcendentals=0),
        compiler_params=pltpu.CompilerParams(vmem_limit_bytes=GRANT),
        name="number",
    )()
    taken = {
        "normal": wall_normal, "ref": sample_ref, "relax": relax.reshape(1, 27),
        "solid": solid, "scell": stencil_cell, "sweight": stencil_weight,
    }
    passed = [taken[name] for name in THROUGH]
    cells, *passed = pl.pallas_call(
        live_kernel,
        out_shape=[jax.ShapeDtypeStruct(v.shape, v.dtype) for v in (number, *passed)],
        in_specs=[VMEM, pl.BlockSpec(memory_space=pltpu.SMEM)] + [VMEM] * (1 + len(passed)),
        out_specs=[VMEM] * (1 + len(passed)),
        compiler_params=pltpu.CompilerParams(vmem_limit_bytes=GRANT),
        name="live",
    )(number, wall_count, wall_cell, *passed)
    taken.update(zip(THROUGH, passed))
    y_even, y_odd, samples, state, early, maps = pl.pallas_call(
        lambda *refs: first_kernel(*refs, gy="gy"),
        out_shape=[
            jax.ShapeDtypeStruct(face, f32),
            jax.ShapeDtypeStruct(face, f32),
            jax.ShapeDtypeStruct((lines, LANES), f32),
            jax.ShapeDtypeStruct((PLANES, *block), f32),
            jax.ShapeDtypeStruct((11, ROWS, LANES), f32),
            jax.ShapeDtypeStruct((3, *block), f32),
        ],
        in_specs=[VMEM] * 8,
        out_specs=[VMEM] * 6,
        compiler_params=pltpu.CompilerParams(vmem_limit_bytes=GRANT),
        name="first",
    )(cells, *taken.values(), populations)

    def swap(value, odd):
        return lax.ppermute(value, "gy", [(i, (((i - odd) ^ 1) + odd) % peers) for i in range(peers)])

    got_far = []
    for n in range(2, peers - 1):
        got_far.append(lax.ppermute(samples, "gy", [(i, (i + n) % peers) for i in range(peers)]))
    y_odd = swap(y_odd, 1)
    y_even = swap(y_even, 0)
    ring = [(i, (i + 1) % devices) for i in range(devices)]
    early = lax.ppermute(early, "gx", ring)
    post, edge, plus, minus = pl.pallas_call(
        lambda *refs: second_kernel(*refs, gy="gy", peers=peers, slots=slots, slots_each=slots_each),
        out_shape=[
            jax.ShapeDtypeStruct(populations.shape, f32),
            jax.ShapeDtypeStruct((up(20 * size_x), LANES), f32),
            jax.ShapeDtypeStruct((4, ROWS, LANES), f32),
            jax.ShapeDtypeStruct((11, ROWS, LANES), f32),
        ],
        in_specs=[VMEM] * (5 + len(got_far)),
        out_specs=[VMEM] * 4,
        compiler_params=pltpu.CompilerParams(vmem_limit_bytes=GRANT),
        name="second",
    )(samples, y_even, y_odd, state, maps, *got_far)
    from_below = lax.ppermute(plus, "gx", ring)
    from_above = lax.ppermute(minus, "gx", [(i, (i - 1) % devices) for i in range(devices)])
    held = pl.pallas_call(
        inner_kernel,
        out_shape=jax.ShapeDtypeStruct(populations.shape, f32),
        in_specs=[VMEM] * 3,
        out_specs=HBM,
        scratch_shapes=[pltpu.VMEM(populations.shape, f32), pltpu.SemaphoreType.DMA((3,))],
        compiler_params=pltpu.CompilerParams(vmem_limit_bytes=GRANT),
        name="inner",
    )(post, edge, maps)
    return pl.pallas_call(
        outer_kernel,
        out_shape=jax.ShapeDtypeStruct(populations.shape, f32),
        in_specs=[VMEM] * 4 + [HBM],
        out_specs=HBM,
        input_output_aliases={4: 0},
        scratch_shapes=[pltpu.VMEM((18, ROWS, LANES), f32), pltpu.SemaphoreType.DMA((2,))],
        compiler_params=pltpu.CompilerParams(vmem_limit_bytes=GRANT),
        name="outer",
    )(post, early, from_below, from_above, pltpu.with_memory_space_constraint(held, pltpu.HBM))


def solution(mesh):
    return jax.shard_map(
        local,
        mesh=mesh,
        in_specs=(
            P(None, "gx", "gy", None),
            P(),
            P("gx", "gy", None),
            P("gx", "gy", None),
            P("gx", "gy", None),
            P("gx", "gy"),
            P("gx", "gy", None),
            P("gx", "gy", None, None),
            P("gx", "gy", None, None),
        ),
        out_specs=P(None, "gx", "gy", None),
        check_vma=False,
    )
```

```python
import jax
import jax.numpy as jnp
from jax import lax
from jax.experimental import pallas as pl
from jax.experimental.pallas import tpu as pltpu
from jax.sharding import PartitionSpec as P


wall_ratio = (1.0 / 9.0) ** (1.0 / 7.0)
LANES = 128
ROWS = 8
RHO, VEL, PLANES = 27, 28, 31
REF, AXIS, SOLID = 0, 1, 2
FACE = 16
HBM = pl.BlockSpec(memory_space=pltpu.HBM)
VMEM = pl.BlockSpec(memory_space=pltpu.VMEM)
THROUGH = ("normal", "ref", "relax")
COVER = 4 * 10**9
GRANT = 4 * 1024 * 1024


def direction(a, b, c):
    return 9 * a + 3 * b + c


def up(n):
    return -(-n // ROWS) * ROWS


def equilibria(density, velocity, wanted):
    ux, uy, uz = velocity
    rest = density * (1.0 - 1.5 * (ux * ux + uy * uy + uz * uz))
    out = {}
    for i in wanted:
        if i in out:
            continue
        step = (i // 9 - 1, i // 3 % 3 - 1, i % 3 - 1)
        along = None
        for s, u in zip(step, (ux, uy, uz)):
            if s:
                along = (u if s > 0 else -u) if along is None else (along + u if s > 0 else along - u)
        if along is None:
            out[i] = rest
            continue
        linear = density * along
        square = rest + 4.5 * (linear * along)
        out[i] = square + 3.0 * linear
        if 26 - i in wanted:
            out[26 - i] = square - 3.0 * linear
    return out


def along_axes(values, triple):
    for stride in (1, 3, 9):
        fresh = list(values)
        for i in range(27):
            if i // stride % 3 == 0:
                fresh[i], fresh[i + stride], fresh[i + 2 * stride] = triple(
                    values[i], values[i + stride], values[i + 2 * stride]
                )
        values = fresh
    return values


def relaxed(pops, keep):
    single = (1.0 / 6.0, 2.0 / 3.0, 1.0 / 6.0)
    weight = [single[i // 9] * single[i // 3 % 3] * single[i % 3] for i in range(27)]

    def raw(m, z, p):
        s = m + p
        return s + z, p - m, s

    def undo(m0, m1, m2):
        return m2 - m1, m0 - m2, m1 + m2

    moment = along_axes([w * p for w, p in zip(weight, pops)], raw)
    density = moment[0]
    inv = 1.0 / density
    vel = [moment[9] * inv, moment[3] * inv, moment[1] * inv]
    first = [moment[9], moment[3], moment[1]]
    second = [4.5 * (j * u) for j, u in zip(first, vel)]
    rest = density - (1.0 / 3.0) * (second[0] + second[1] + second[2])
    mu, nu, ka = (1.0, 0.0, 1.0 / 3.0), (0.0, 1.0 / 3.0, 0.0), (1.0 / 3.0, 0.0, 1.0 / 3.0)
    cross = {}
    kept = []
    for i in range(27):
        p = (i // 9, i // 3 % 3, i % 3)
        eq = None
        terms = [(mu[p[0]] * mu[p[1]] * mu[p[2]], rest)]
        for d in range(3):
            o, q = [e for e in range(3) if e != d]
            terms.append((3.0 * nu[p[d]] * mu[p[o]] * mu[p[q]], first[d]))
            terms.append((ka[p[d]] * mu[p[o]] * mu[p[q]], second[d]))
            factor = 9.0 * nu[p[o]] * nu[p[q]] * mu[p[d]]
            if factor:
                if d not in cross:
                    cross[d] = first[o] * vel[q]
                terms.append((factor, cross[d]))
        for f, t in terms:
            if f:
                t = t if abs(f - 1.0) < 1e-12 else f * t
                eq = t if eq is None else eq + t
        dev = moment[i] if eq is None else moment[i] - eq
        kept.append(keep[i] * dev)
    back = (3.0, 1.5, 3.0)
    kept = along_axes(kept, undo)
    kept = [back[i // 9] * back[i // 3 % 3] * back[i % 3] * k for i, k in enumerate(kept)]
    return density, vel, kept


def lanes_of(table, index):
    return jnp.take_along_axis(table, index, axis=1, mode="promise_in_bounds")


def number_kernel(out):
    out[...] = lax.broadcasted_iota(jnp.int32, out.shape, 1)


def live_kernel(number, count, cell, *rest):
    half = (len(rest) - 1) // 2
    rest[half][...] = jnp.where(number[...] < count[0, 0], cell[0], -1)
    for source, target in zip(rest[:half], rest[half + 1 :]):
        target[...] = source[...]


def cell_kernel(relax, pop, scell, sweight, state_o, sample_o):
    size_x, slots = pop.shape[1], scell.shape[-1]
    rates = [1.0 - jnp.broadcast_to(relax[0:1, i : i + 1], (ROWS, LANES)) for i in range(27)]
    velocity = []
    for x in range(size_x):
        density, vel, kept = relaxed([pop[i, x] for i in range(27)], rates)
        velocity.append(vel)
        for i in range(27):
            state_o[i, x] = kept[i]
        state_o[RHO, x] = density
        for d in range(3):
            state_o[VEL + d, x] = vel[d]
    sub = lax.broadcasted_iota(jnp.int32, (ROWS, LANES), 0)
    for t in range(slots // LANES):
        cells = scell[0, 0, :, t * LANES : (t + 1) * LANES]
        weights = sweight[0, 0, :, t * LANES : (t + 1) * LANES]
        row, z = cells // LANES, cells % LANES
        low = jnp.broadcast_to(z[0:1], (ROWS, LANES))
        other = z != low
        high = jnp.max(jnp.where(other, z, 0), axis=0, keepdims=True)
        high = jnp.broadcast_to(high, (ROWS, LANES))
        w_high = jnp.where(other, weights, 0.0)
        w_low = weights - w_high
        total = [None] * 3
        for x in range(size_x):
            a_low = jnp.zeros((ROWS, LANES), jnp.float32)
            a_high = a_low
            for k in range(8):
                hit = jnp.broadcast_to(row[k : k + 1], (ROWS, LANES)) == sub + x * ROWS
                a_low += jnp.where(hit, jnp.broadcast_to(w_low[k : k + 1], (ROWS, LANES)), 0.0)
                a_high += jnp.where(hit, jnp.broadcast_to(w_high[k : k + 1], (ROWS, LANES)), 0.0)
            for d in range(3):
                part = a_low * lanes_of(velocity[x][d], low) + a_high * lanes_of(velocity[x][d], high)
                total[d] = part if total[d] is None else total[d] + part
        for d in range(3):
            r = d * (slots // LANES) + t
            sample_o[r : r + 1, :] = jnp.sum(total[d], axis=0, keepdims=True)


def face_kernel(cell, normal, ref, solid, state, sample, even_o, odd_o, early_o, map_o, *, gy):
    size_x, walls = solid.shape[0], cell.shape[-1]
    row = jnp.where(cell[...] < 0, -1, cell[...] // LANES)
    z = cell[...] % LANES
    low = (ref[0] % LANES + 1).astype(jnp.float32)
    high = (ref[0] // LANES * 4 + normal[0] // 2).astype(jnp.float32)
    height = size_x * ROWS
    at = lax.broadcasted_iota(jnp.int32, (height, walls), 0) == jnp.broadcast_to(row, (height, walls))
    left = jnp.concatenate(
        [jnp.where(at, jnp.broadcast_to(v, (height, walls)), 0.0) for v in (low, high)], axis=0
    ).astype(jnp.bfloat16)
    hot = lax.broadcasted_iota(jnp.int32, (LANES, walls), 0) == jnp.broadcast_to(z, (LANES, walls))
    hot = jnp.where(hot, 1.0, 0.0).astype(jnp.bfloat16)
    dense = lax.dot_general(left, hot, (((1,), (1,)), ((), ())), preferred_element_type=jnp.float32)
    for x in range(size_x):
        low = dense[x * ROWS : (x + 1) * ROWS].astype(jnp.int32)
        high = dense[height + x * ROWS : height + (x + 1) * ROWS].astype(jnp.int32)
        map_o[REF, x] = ((high // 4) * LANES + low - 1).astype(jnp.float32)
        map_o[AXIS, x] = (high % 4).astype(jnp.float32)
        map_o[SOLID, x] = solid[x].astype(jnp.float32)
    for n in range(9):
        early_o[n] = state[18 + n, size_x - 1]
    early_o[9] = state[RHO, size_x - 1]
    early_o[10] = map_o[SOLID, size_x - 1]
    base = sample.shape[0]
    even_o[:base, :] = sample[...]
    parity = lax.axis_index(gy) % 2
    faces = []
    for b, y in ((2, ROWS - 1), (0, 0)):
        planes = [(state, direction(a, b, c)) for a in range(3) for c in range(3)]
        planes += [(state, n) for n in range(RHO, PLANES)] + [(map_o, n) for n in range(3)]
        faces.append([array[plane, x, y : y + 1, :] for array, plane in planes for x in range(size_x)])
    for n, (above, below) in enumerate(zip(*faces)):
        even_o[base + n : base + n + 1, :] = jnp.where(parity == 0, above, below)
        odd_o[n : n + 1, :] = jnp.where(parity == 0, below, above)


def first_kernel(
    cells, normal, ref, relax, solid, scell, sweight, pop, even_o, odd_o, sample_o, state_o, early_o, map_o, *, gy
):
    cell_kernel(relax, pop, scell, sweight, state_o, sample_o)
    face_kernel(cells, normal, ref, solid, state_o, sample_o, even_o, odd_o, early_o, map_o, gy=gy)


def owners(own, y_even, s_odd, far, gy, peers):
    me = lax.axis_index(gy)
    below, above = (me + peers - 1) % peers, (me + 1) % peers
    even = me % 2 == 0
    tables = [(own, me), (y_even, jnp.where(even, above, below)), (s_odd, jnp.where(even, below, above))]
    tables += [(table, (me + peers - (n + 2)) % peers) for n, table in enumerate(far)]
    return tables, me, below, above


def walled(tables, block, width, slots_each, ref, axis, vel):
    index = jnp.maximum(ref, 0)
    source = index // slots_each
    lane = block(lambda p: p * slots_each % LANES) + index % slots_each
    out = []
    for d in range(3):
        picked = jnp.zeros(ref.shape, jnp.float32)
        for table, who in tables:

            def line(p):
                return jnp.broadcast_to(table[pl.ds(d * width + p * slots_each // LANES, 1), :], (ROWS, LANES))

            picked = jnp.where(source == who, lanes_of(block(line), lane), picked)
        tangential = jnp.where(axis == d, 0.0, wall_ratio * picked)
        out.append(jnp.where(ref >= 0, tangential, vel[d]))
    return out


def beside(y_even, y_odd, gy, base, size_x):
    even = lax.axis_index(gy) % 2 == 0
    sub = lax.broadcasted_iota(jnp.int32, (ROWS, LANES), 0)

    def plane(n):
        got = (y_odd[pl.ds(n * size_x, size_x), :], y_even[pl.ds(base + n * size_x, size_x), :])
        tile = None
        for side in range(2):
            picked = jnp.where(even, got[side], got[1 - side])
            for x in range(size_x):
                row = jnp.broadcast_to(picked[x : x + 1], (ROWS, LANES))
                tile = row if tile is None else jnp.where(sub == side * size_x + x, row, tile)
        return tile

    return plane, sub


def second_kernel(own, y_even, y_odd, s_odd, state, maps, *rest, gy, peers, slots, slots_each):
    far, (plus_o, minus_o, vel_o, halo_o) = rest[: peers - 3], rest[peers - 3 :]
    size_x, width = maps.shape[1], slots // LANES
    tables, me, below, above = owners(own, y_even, s_odd, far, gy, peers)
    plane, sub = beside(y_even, y_odd, gy, up(3 * width), size_x)
    first_side = sub < size_x
    for x in range(size_x):
        ref, axis = maps[REF, x].astype(jnp.int32), maps[AXIS, x].astype(jnp.int32)
        vel = [state[VEL + d, x] for d in range(3)]
        vel = walled(tables, lambda f: f(me), width, slots_each, ref, axis, vel)
        for d in range(3):
            vel_o[d, x] = vel[d]
            if x == size_x - 1:
                plus_o[d] = vel[d]
        if x == 0:
            eq = equilibria(state[RHO, x], vel, range(9))
            for i in range(9):
                minus_o[i] = state[i, x] + eq[i]
            minus_o[9] = maps[SOLID, x]
    ref, axis = plane(13).astype(jnp.int32), plane(14).astype(jnp.int32)
    vel = [plane(10 + d) for d in range(3)]
    vel = walled(tables, lambda f: jnp.where(first_side, f(below), f(above)), width, slots_each, ref, axis, vel)
    vel[1] = jnp.where(first_side, vel[1], -vel[1])
    for d in range(3):
        halo_o[d] = vel[d]
    eq = equilibria(plane(9), vel, [direction(a, 2, c) for a in (0, 2) for c in range(3)])
    solid = plane(15)
    for o, a, x, last in ((plus_o, 2, size_x - 1, 3), (minus_o, 0, 0, 10)):
        corner = [plane(3 * a + c) + eq[direction(a, 2, c)] for c in range(3)] + [solid]
        for side in range(2):
            r = side * size_x + x
            for n in range(4):
                o[last, side * 4 + n : side * 4 + n + 1, :] = corner[n][r : r + 1]


def third_kernel(y_even, y_odd, state, vel, halo, post_o, edge_o, *, gy, slots):
    size_x = post_o.shape[1]
    plane, _ = beside(y_even, y_odd, gy, up(3 * (slots // LANES)), size_x)
    for x in range(size_x):
        eq = equilibria(state[RHO, x], [vel[d, x] for d in range(3)], range(27))
        for i in range(27):
            post_o[i, x] = state[i, x] + eq[i]
    wanted = [direction(a, 2, c) for a in range(3) for c in range(3)]
    eq = equilibria(plane(9), [halo[d] for d in range(3)], wanted)
    for n, value in enumerate([plane(n) + eq[i] for n, i in enumerate(wanted)] + [plane(15)]):
        for side in range(2):
            r = (side * 10 + n) * size_x
            edge_o[r : r + size_x, :] = value[side * size_x : (side + 1) * size_x]


def shifted(tile, row, step_y):
    if step_y == 0:
        return tile
    sub = lax.broadcasted_iota(jnp.int32, (ROWS, LANES), 0)
    rolled = pltpu.roll(tile, step_y % ROWS, 0)
    return jnp.where(sub == (0 if step_y > 0 else ROWS - 1), jnp.broadcast_to(row, (ROWS, LANES)), rolled)


def along_z(tile, c):
    return tile if c == 1 else pltpu.roll(tile, (c - 1) % LANES, 1)


def inner_kernel(post, edge, maps, out_h, out, sems):
    size_x = post.shape[1]
    copies = []
    for a in (1, 2, 0):
        first, last = max(a - 1, 0), size_x + min(a - 1, 0)
        for b in range(3):
            side = 0 if b == 2 else 1
            for x in range(first, last):
                q = x - (a - 1)

                def row(n):
                    r = (side * 10 + n) * size_x + q
                    return edge[r : r + 1, :]

                wall = shifted(maps[SOLID, q], row(9), b - 1)
                for c in range(3):
                    i = direction(a, b, c)
                    moved = along_z(shifted(post[i, q], row(3 * a + c), b - 1), c)
                    out[i, x] = jnp.where(along_z(wall, c) > 0.5, post[26 - i, x], moved)
        part = (pl.ds(9 * a, 9), pl.ds(first, last - first))
        copy = pltpu.make_async_copy(out.at[part], out_h.at[part], sems.at[a])
        copy.start()
        copies.append(copy)
    for copy in copies:
        copy.wait()


def outer_kernel(post, early, below, above, held_h, out_h, out, sems):
    del held_h
    size_x = post.shape[1]
    copies = []
    for a, x in ((0, size_x - 1), (2, 0)):
        if a == 0:
            tiles, solid, corner = [above[n] for n in range(9)], above[9], above[10]
        else:
            eq = equilibria(early[9], [below[d] for d in range(3)], range(18, 27))
            tiles, solid, corner = [early[n] + eq[18 + n] for n in range(9)], early[10], below[3]
        for b in range(3):
            side = 0 if b == 2 else 1
            wall = shifted(solid, corner[side * 4 + 3 : side * 4 + 4], b - 1)
            for c in range(3):
                i = direction(a, b, c)
                moved = shifted(tiles[3 * b + c], corner[side * 4 + c : side * 4 + c + 1], b - 1)
                moved = along_z(moved, c)
                out[i % 9 + 9 * (a // 2)] = jnp.where(along_z(wall, c) > 0.5, post[26 - i, x], moved)
        copy = pltpu.make_async_copy(out.at[pl.ds(9 * (a // 2), 9)], out_h.at[pl.ds(9 * a, 9), x], sems.at[a // 2])
        copy.start()
        copies.append(copy)
    for copy in copies:
        copy.wait()


def local(
    populations, relax, solid, wall_cell, wall_normal, wall_count, sample_ref, stencil_cell, stencil_weight
):
    _, size_x, size_y, size_z = populations.shape
    walls, slots = wall_cell.shape[-1], stencil_cell.shape[-1]
    devices, peers = lax.axis_size("gx"), lax.axis_size("gy")
    slots_each = slots // peers
    if (size_y, size_z) != (ROWS, LANES) or walls % LANES or slots % LANES:
        raise ValueError("unsupported block")
    if LANES % slots_each or peers % 2 or peers < 4 or 2 * size_x > ROWS:
        raise ValueError("unsupported mesh")
    f32 = jnp.float32
    lines = up(3 * (slots // LANES))
    face = (lines + FACE * size_x, LANES)
    block = (size_x, ROWS, LANES)
    number = pl.pallas_call(
        number_kernel,
        out_shape=jax.ShapeDtypeStruct((1, walls), jnp.int32),
        out_specs=VMEM,
        cost_estimate=pl.CostEstimate(flops=COVER, bytes_accessed=0, transcendentals=0),
        compiler_params=pltpu.CompilerParams(vmem_limit_bytes=GRANT),
        name="number",
    )()
    taken = {
        "normal": wall_normal, "ref": sample_ref, "relax": relax.reshape(1, 27),
        "solid": solid, "scell": stencil_cell, "sweight": stencil_weight,
    }
    passed = [taken[name] for name in THROUGH]
    cells, *passed = pl.pallas_call(
        live_kernel,
        out_shape=[jax.ShapeDtypeStruct(v.shape, v.dtype) for v in (number, *passed)],
        in_specs=[VMEM, pl.BlockSpec(memory_space=pltpu.SMEM)] + [VMEM] * (1 + len(passed)),
        out_specs=[VMEM] * (1 + len(passed)),
        compiler_params=pltpu.CompilerParams(vmem_limit_bytes=GRANT),
        name="live",
    )(number, wall_count, wall_cell, *passed)
    taken.update(zip(THROUGH, passed))
    y_even, y_odd, samples, state, early, maps = pl.pallas_call(
        lambda *refs: first_kernel(*refs, gy="gy"),
        out_shape=[
            jax.ShapeDtypeStruct(face, f32),
            jax.ShapeDtypeStruct((FACE * size_x, LANES), f32),
            jax.ShapeDtypeStruct((lines, LANES), f32),
            jax.ShapeDtypeStruct((PLANES, *block), f32),
            jax.ShapeDtypeStruct((11, ROWS, LANES), f32),
            jax.ShapeDtypeStruct((3, *block), f32),
        ],
        in_specs=[VMEM] * 8,
        out_specs=[VMEM] * 6,
        compiler_params=pltpu.CompilerParams(vmem_limit_bytes=GRANT),
        name="first",
    )(cells, *taken.values(), populations)

    def swap(value, odd):
        return lax.ppermute(value, "gy", [(i, (((i - odd) ^ 1) + odd) % peers) for i in range(peers)])

    got_far = []
    for n in range(2, peers - 1) if peers != 4 else ():
        got_far.append(lax.ppermute(samples, "gy", [(i, (i + n) % peers) for i in range(peers)]))
    s_odd = swap(samples, 1)
    y_odd = swap(y_odd, 1)
    y_even = swap(y_even, 0)
    if peers == 4:
        got_far = [swap(s_odd, 0)]
    ring = [(i, (i + 1) % devices) for i in range(devices)]
    early = lax.ppermute(early, "gx", ring)
    plus, minus, vel, halo = pl.pallas_call(
        lambda *refs: second_kernel(*refs, gy="gy", peers=peers, slots=slots, slots_each=slots_each),
        out_shape=[
            jax.ShapeDtypeStruct((4, ROWS, LANES), f32),
            jax.ShapeDtypeStruct((11, ROWS, LANES), f32),
            jax.ShapeDtypeStruct((3, *block), f32),
            jax.ShapeDtypeStruct((3, ROWS, LANES), f32),
        ],
        in_specs=[VMEM] * (6 + len(got_far)),
        out_specs=[VMEM] * 4,
        compiler_params=pltpu.CompilerParams(vmem_limit_bytes=GRANT),
        name="second",
    )(samples, y_even, y_odd, s_odd, state, maps, *got_far)
    post, edge = pl.pallas_call(
        lambda *refs: third_kernel(*refs, gy="gy", slots=slots),
        out_shape=[jax.ShapeDtypeStruct(populations.shape, f32), jax.ShapeDtypeStruct((up(20 * size_x), LANES), f32)],
        in_specs=[VMEM] * 5,
        out_specs=[VMEM] * 2,
        compiler_params=pltpu.CompilerParams(vmem_limit_bytes=GRANT),
        name="third",
    )(y_even, y_odd, state, vel, halo)
    from_below = lax.ppermute(plus, "gx", ring)
    from_above = lax.ppermute(minus, "gx", [(i, (i - 1) % devices) for i in range(devices)])
    held = pl.pallas_call(
        inner_kernel,
        out_shape=jax.ShapeDtypeStruct(populations.shape, f32),
        in_specs=[VMEM] * 3,
        out_specs=HBM,
        scratch_shapes=[pltpu.VMEM(populations.shape, f32), pltpu.SemaphoreType.DMA((3,))],
        compiler_params=pltpu.CompilerParams(vmem_limit_bytes=GRANT),
        name="inner",
    )(post, edge, maps)
    return pl.pallas_call(
        outer_kernel,
        out_shape=jax.ShapeDtypeStruct(populations.shape, f32),
        in_specs=[VMEM] * 4 + [HBM],
        out_specs=HBM,
        input_output_aliases={4: 0},
        scratch_shapes=[pltpu.VMEM((18, ROWS, LANES), f32), pltpu.SemaphoreType.DMA((2,))],
        compiler_params=pltpu.CompilerParams(vmem_limit_bytes=GRANT),
        name="outer",
    )(post, early, from_below, from_above, pltpu.with_memory_space_constraint(held, pltpu.HBM))


def solution(mesh):
    return jax.shard_map(
        local,
        mesh=mesh,
        in_specs=(
            P(None, "gx", "gy", None),
            P(),
            P("gx", "gy", None),
            P("gx", "gy", None),
            P("gx", "gy", None),
            P("gx", "gy"),
            P("gx", "gy", None),
            P("gx", "gy", None, None),
            P("gx", "gy", None, None),
        ),
        out_specs=P(None, "gx", "gy", None),
        check_vma=False,
    )
```

```python
import jax
import jax.numpy as jnp
from jax import lax
from jax.experimental import pallas as pl
from jax.experimental.pallas import tpu as pltpu
from jax.sharding import PartitionSpec as P


wall_ratio = (1.0 / 9.0) ** (1.0 / 7.0)
LANES = 128
ROWS = 8
RHO, VEL, PLANES = 27, 28, 31
REF, AXIS, SOLID = 0, 1, 2
FACE = 16
HBM = pl.BlockSpec(memory_space=pltpu.HBM)
VMEM = pl.BlockSpec(memory_space=pltpu.VMEM)
THROUGH = ("normal", "ref", "relax")
COVER = 4 * 10**9
GRANT = 4 * 1024 * 1024


def direction(a, b, c):
    return 9 * a + 3 * b + c


def up(n):
    return -(-n // ROWS) * ROWS


def equilibria(density, velocity, wanted):
    ux, uy, uz = velocity
    rest = density * (1.0 - 1.5 * (ux * ux + uy * uy + uz * uz))
    out = {}
    for i in wanted:
        if i in out:
            continue
        step = (i // 9 - 1, i // 3 % 3 - 1, i % 3 - 1)
        along = None
        for s, u in zip(step, (ux, uy, uz)):
            if s:
                along = (u if s > 0 else -u) if along is None else (along + u if s > 0 else along - u)
        if along is None:
            out[i] = rest
            continue
        linear = density * along
        square = rest + 4.5 * (linear * along)
        out[i] = square + 3.0 * linear
        if 26 - i in wanted:
            out[26 - i] = square - 3.0 * linear
    return out


def along_axes(values, triple):
    for stride in (1, 3, 9):
        fresh = list(values)
        for i in range(27):
            if i // stride % 3 == 0:
                fresh[i], fresh[i + stride], fresh[i + 2 * stride] = triple(
                    values[i], values[i + stride], values[i + 2 * stride]
                )
        values = fresh
    return values


def relaxed(pops, keep):
    single = (1.0 / 6.0, 2.0 / 3.0, 1.0 / 6.0)
    weight = [single[i // 9] * single[i // 3 % 3] * single[i % 3] for i in range(27)]

    def raw(m, z, p):
        s = m + p
        return s + z, p - m, s

    def undo(m0, m1, m2):
        return m2 - m1, m0 - m2, m1 + m2

    moment = along_axes([w * p for w, p in zip(weight, pops)], raw)
    density = moment[0]
    inv = 1.0 / density
    vel = [moment[9] * inv, moment[3] * inv, moment[1] * inv]
    first = [moment[9], moment[3], moment[1]]
    second = [4.5 * (j * u) for j, u in zip(first, vel)]
    rest = density - (1.0 / 3.0) * (second[0] + second[1] + second[2])
    mu, nu, ka = (1.0, 0.0, 1.0 / 3.0), (0.0, 1.0 / 3.0, 0.0), (1.0 / 3.0, 0.0, 1.0 / 3.0)
    cross = {}
    kept = []
    for i in range(27):
        p = (i // 9, i // 3 % 3, i % 3)
        eq = None
        terms = [(mu[p[0]] * mu[p[1]] * mu[p[2]], rest)]
        for d in range(3):
            o, q = [e for e in range(3) if e != d]
            terms.append((3.0 * nu[p[d]] * mu[p[o]] * mu[p[q]], first[d]))
            terms.append((ka[p[d]] * mu[p[o]] * mu[p[q]], second[d]))
            factor = 9.0 * nu[p[o]] * nu[p[q]] * mu[p[d]]
            if factor:
                if d not in cross:
                    cross[d] = first[o] * vel[q]
                terms.append((factor, cross[d]))
        for f, t in terms:
            if f:
                t = t if abs(f - 1.0) < 1e-12 else f * t
                eq = t if eq is None else eq + t
        dev = moment[i] if eq is None else moment[i] - eq
        kept.append(keep[i] * dev)
    back = (3.0, 1.5, 3.0)
    kept = along_axes(kept, undo)
    kept = [back[i // 9] * back[i // 3 % 3] * back[i % 3] * k for i, k in enumerate(kept)]
    return density, vel, kept


def lanes_of(table, index):
    return jnp.take_along_axis(table, index, axis=1, mode="promise_in_bounds")


def number_kernel(out):
    out[...] = lax.broadcasted_iota(jnp.int32, out.shape, 1)


def live_kernel(number, count, cell, *rest):
    half = (len(rest) - 1) // 2
    rest[half][...] = jnp.where(number[...] < count[0, 0], cell[0], -1)
    for source, target in zip(rest[:half], rest[half + 1 :]):
        target[...] = source[...]


def cell_kernel(relax, pop, scell, sweight, state_o, sample_o):
    size_x, slots = pop.shape[1], scell.shape[-1]
    rates = [1.0 - jnp.broadcast_to(relax[0:1, i : i + 1], (ROWS, LANES)) for i in range(27)]
    velocity = []
    for x in range(size_x):
        density, vel, kept = relaxed([pop[i, x] for i in range(27)], rates)
        velocity.append(vel)
        for i in range(27):
            state_o[i, x] = kept[i]
        state_o[RHO, x] = density
        for d in range(3):
            state_o[VEL + d, x] = vel[d]
    sub = lax.broadcasted_iota(jnp.int32, (ROWS, LANES), 0)
    for t in range(slots // LANES):
        cells = scell[0, 0, :, t * LANES : (t + 1) * LANES]
        weights = sweight[0, 0, :, t * LANES : (t + 1) * LANES]
        row, z = cells // LANES, cells % LANES
        low = jnp.broadcast_to(z[0:1], (ROWS, LANES))
        other = z != low
        high = jnp.max(jnp.where(other, z, 0), axis=0, keepdims=True)
        high = jnp.broadcast_to(high, (ROWS, LANES))
        w_high = jnp.where(other, weights, 0.0)
        w_low = weights - w_high
        total = [None] * 3
        for x in range(size_x):
            a_low = jnp.zeros((ROWS, LANES), jnp.float32)
            a_high = a_low
            for k in range(8):
                hit = jnp.broadcast_to(row[k : k + 1], (ROWS, LANES)) == sub + x * ROWS
                a_low += jnp.where(hit, jnp.broadcast_to(w_low[k : k + 1], (ROWS, LANES)), 0.0)
                a_high += jnp.where(hit, jnp.broadcast_to(w_high[k : k + 1], (ROWS, LANES)), 0.0)
            for d in range(3):
                part = a_low * lanes_of(velocity[x][d], low) + a_high * lanes_of(velocity[x][d], high)
                total[d] = part if total[d] is None else total[d] + part
        for d in range(3):
            r = d * (slots // LANES) + t
            sample_o[r : r + 1, :] = jnp.sum(total[d], axis=0, keepdims=True)


def face_kernel(cell, normal, ref, solid, state, sample, even_o, odd_o, early_o, map_o, *, gy):
    size_x, walls = solid.shape[0], cell.shape[-1]
    row = jnp.where(cell[...] < 0, -1, cell[...] // LANES)
    z = cell[...] % LANES
    low = (ref[0] % LANES + 1).astype(jnp.float32)
    high = (ref[0] // LANES * 4 + normal[0] // 2).astype(jnp.float32)
    height = size_x * ROWS
    at = lax.broadcasted_iota(jnp.int32, (height, walls), 0) == jnp.broadcast_to(row, (height, walls))
    left = jnp.concatenate(
        [jnp.where(at, jnp.broadcast_to(v, (height, walls)), 0.0) for v in (low, high)], axis=0
    ).astype(jnp.bfloat16)
    hot = lax.broadcasted_iota(jnp.int32, (LANES, walls), 0) == jnp.broadcast_to(z, (LANES, walls))
    hot = jnp.where(hot, 1.0, 0.0).astype(jnp.bfloat16)
    dense = lax.dot_general(left, hot, (((1,), (1,)), ((), ())), preferred_element_type=jnp.float32)
    for x in range(size_x):
        low = dense[x * ROWS : (x + 1) * ROWS].astype(jnp.int32)
        high = dense[height + x * ROWS : height + (x + 1) * ROWS].astype(jnp.int32)
        map_o[REF, x] = ((high // 4) * LANES + low - 1).astype(jnp.float32)
        map_o[AXIS, x] = (high % 4).astype(jnp.float32)
        map_o[SOLID, x] = solid[x].astype(jnp.float32)
    for n in range(9):
        early_o[n] = state[18 + n, size_x - 1]
    early_o[9] = state[RHO, size_x - 1]
    early_o[10] = map_o[SOLID, size_x - 1]
    base = sample.shape[0]
    even_o[:base, :] = sample[...]
    odd_o[:base, :] = sample[...]
    parity = lax.axis_index(gy) % 2
    faces = []
    for b, y in ((2, ROWS - 1), (0, 0)):
        planes = [(state, direction(a, b, c)) for a in range(3) for c in range(3)]
        planes += [(state, n) for n in range(RHO, PLANES)] + [(map_o, n) for n in range(3)]
        faces.append([array[plane, x, y : y + 1, :] for array, plane in planes for x in range(size_x)])
    for n, (above, below) in enumerate(zip(*faces)):
        even_o[base + n : base + n + 1, :] = jnp.where(parity == 0, above, below)
        odd_o[base + n : base + n + 1, :] = jnp.where(parity == 0, below, above)


def first_kernel(
    cells, normal, ref, relax, solid, scell, sweight, pop, even_o, odd_o, sample_o, state_o, early_o, map_o, *, gy
):
    cell_kernel(relax, pop, scell, sweight, state_o, sample_o)
    face_kernel(cells, normal, ref, solid, state_o, sample_o, even_o, odd_o, early_o, map_o, gy=gy)


def owners(own, y_even, y_odd, far, gy, peers):
    me = lax.axis_index(gy)
    below, above = (me + peers - 1) % peers, (me + 1) % peers
    even = me % 2 == 0
    tables = [(own, me), (y_even, jnp.where(even, above, below)), (y_odd, jnp.where(even, below, above))]
    tables += [(table, (me + peers - (n + 2)) % peers) for n, table in enumerate(far)]
    return tables, me, below, above


def walled(tables, block, width, slots_each, ref, axis, vel):
    index = jnp.maximum(ref, 0)
    source = index // slots_each
    lane = block(lambda p: p * slots_each % LANES) + index % slots_each
    out = []
    for d in range(3):
        picked = jnp.zeros(ref.shape, jnp.float32)
        for table, who in tables:

            def line(p):
                return jnp.broadcast_to(table[pl.ds(d * width + p * slots_each // LANES, 1), :], (ROWS, LANES))

            picked = jnp.where(source == who, lanes_of(block(line), lane), picked)
        tangential = jnp.where(axis == d, 0.0, wall_ratio * picked)
        out.append(jnp.where(ref >= 0, tangential, vel[d]))
    return out


def beside(y_even, y_odd, gy, base, size_x):
    even = lax.axis_index(gy) % 2 == 0
    sub = lax.broadcasted_iota(jnp.int32, (ROWS, LANES), 0)

    def plane(n):
        rows = pl.ds(base + n * size_x, size_x)
        got = (y_odd[rows, :], y_even[rows, :])
        tile = None
        for side in range(2):
            picked = jnp.where(even, got[side], got[1 - side])
            for x in range(size_x):
                row = jnp.broadcast_to(picked[x : x + 1], (ROWS, LANES))
                tile = row if tile is None else jnp.where(sub == side * size_x + x, row, tile)
        return tile

    return plane, sub


def second_kernel(own, y_even, y_odd, state, maps, *rest, gy, peers, slots, slots_each):
    far, (plus_o, minus_o, vel_o, halo_o) = rest[: peers - 3], rest[peers - 3 :]
    size_x, width = maps.shape[1], slots // LANES
    tables, me, below, above = owners(own, y_even, y_odd, far, gy, peers)
    plane, sub = beside(y_even, y_odd, gy, up(3 * width), size_x)
    first_side = sub < size_x
    for x in range(size_x):
        ref, axis = maps[REF, x].astype(jnp.int32), maps[AXIS, x].astype(jnp.int32)
        vel = [state[VEL + d, x] for d in range(3)]
        vel = walled(tables, lambda f: f(me), width, slots_each, ref, axis, vel)
        for d in range(3):
            vel_o[d, x] = vel[d]
            if x == size_x - 1:
                plus_o[d] = vel[d]
        if x == 0:
            eq = equilibria(state[RHO, x], vel, range(9))
            for i in range(9):
                minus_o[i] = state[i, x] + eq[i]
            minus_o[9] = maps[SOLID, x]
    ref, axis = plane(13).astype(jnp.int32), plane(14).astype(jnp.int32)
    vel = [plane(10 + d) for d in range(3)]
    vel = walled(tables, lambda f: jnp.where(first_side, f(below), f(above)), width, slots_each, ref, axis, vel)
    vel[1] = jnp.where(first_side, vel[1], -vel[1])
    for d in range(3):
        halo_o[d] = vel[d]
    eq = equilibria(plane(9), vel, [direction(a, 2, c) for a in (0, 2) for c in range(3)])
    solid = plane(15)
    for o, a, x, last in ((plus_o, 2, size_x - 1, 3), (minus_o, 0, 0, 10)):
        corner = [plane(3 * a + c) + eq[direction(a, 2, c)] for c in range(3)] + [solid]
        for side in range(2):
            r = side * size_x + x
            for n in range(4):
                o[last, side * 4 + n : side * 4 + n + 1, :] = corner[n][r : r + 1]


def third_kernel(y_even, y_odd, state, vel, halo, post_o, edge_o, *, gy, slots):
    size_x = post_o.shape[1]
    plane, _ = beside(y_even, y_odd, gy, up(3 * (slots // LANES)), size_x)
    for x in range(size_x):
        eq = equilibria(state[RHO, x], [vel[d, x] for d in range(3)], range(27))
        for i in range(27):
            post_o[i, x] = state[i, x] + eq[i]
    wanted = [direction(a, 2, c) for a in range(3) for c in range(3)]
    eq = equilibria(plane(9), [halo[d] for d in range(3)], wanted)
    for n, value in enumerate([plane(n) + eq[i] for n, i in enumerate(wanted)] + [plane(15)]):
        for side in range(2):
            r = (side * 10 + n) * size_x
            edge_o[r : r + size_x, :] = value[side * size_x : (side + 1) * size_x]


def shifted(tile, row, step_y):
    if step_y == 0:
        return tile
    sub = lax.broadcasted_iota(jnp.int32, (ROWS, LANES), 0)
    rolled = pltpu.roll(tile, step_y % ROWS, 0)
    return jnp.where(sub == (0 if step_y > 0 else ROWS - 1), jnp.broadcast_to(row, (ROWS, LANES)), rolled)


def along_z(tile, c):
    return tile if c == 1 else pltpu.roll(tile, (c - 1) % LANES, 1)


def inner_kernel(post, edge, maps, out_h, out, sems):
    size_x = post.shape[1]
    copies = []
    for a in (1, 2, 0):
        first, last = max(a - 1, 0), size_x + min(a - 1, 0)
        for b in range(3):
            side = 0 if b == 2 else 1
            for x in range(first, last):
                q = x - (a - 1)

                def row(n):
                    r = (side * 10 + n) * size_x + q
                    return edge[r : r + 1, :]

                wall = shifted(maps[SOLID, q], row(9), b - 1)
                for c in range(3):
                    i = direction(a, b, c)
                    moved = along_z(shifted(post[i, q], row(3 * a + c), b - 1), c)
                    out[i, x] = jnp.where(along_z(wall, c) > 0.5, post[26 - i, x], moved)
        part = (pl.ds(9 * a, 9), pl.ds(first, last - first))
        copy = pltpu.make_async_copy(out.at[part], out_h.at[part], sems.at[a])
        copy.start()
        copies.append(copy)
    for copy in copies:
        copy.wait()


def outer_kernel(post, early, below, above, held_h, out_h, out, sems):
    del held_h
    size_x = post.shape[1]
    copies = []
    for a, x in ((0, size_x - 1), (2, 0)):
        if a == 0:
            tiles, solid, corner = [above[n] for n in range(9)], above[9], above[10]
        else:
            eq = equilibria(early[9], [below[d] for d in range(3)], range(18, 27))
            tiles, solid, corner = [early[n] + eq[18 + n] for n in range(9)], early[10], below[3]
        for b in range(3):
            side = 0 if b == 2 else 1
            wall = shifted(solid, corner[side * 4 + 3 : side * 4 + 4], b - 1)
            for c in range(3):
                i = direction(a, b, c)
                moved = shifted(tiles[3 * b + c], corner[side * 4 + c : side * 4 + c + 1], b - 1)
                moved = along_z(moved, c)
                out[i % 9 + 9 * (a // 2)] = jnp.where(along_z(wall, c) > 0.5, post[26 - i, x], moved)
        copy = pltpu.make_async_copy(out.at[pl.ds(9 * (a // 2), 9)], out_h.at[pl.ds(9 * a, 9), x], sems.at[a // 2])
        copy.start()
        copies.append(copy)
    for copy in copies:
        copy.wait()


def local(
    populations, relax, solid, wall_cell, wall_normal, wall_count, sample_ref, stencil_cell, stencil_weight
):
    _, size_x, size_y, size_z = populations.shape
    walls, slots = wall_cell.shape[-1], stencil_cell.shape[-1]
    devices, peers = lax.axis_size("gx"), lax.axis_size("gy")
    slots_each = slots // peers
    if (size_y, size_z) != (ROWS, LANES) or walls % LANES or slots % LANES:
        raise ValueError("unsupported block")
    if LANES % slots_each or peers % 2 or peers < 4 or 2 * size_x > ROWS:
        raise ValueError("unsupported mesh")
    f32 = jnp.float32
    lines = up(3 * (slots // LANES))
    face = (lines + FACE * size_x, LANES)
    block = (size_x, ROWS, LANES)
    number = pl.pallas_call(
        number_kernel,
        out_shape=jax.ShapeDtypeStruct((1, walls), jnp.int32),
        out_specs=VMEM,
        cost_estimate=pl.CostEstimate(flops=COVER, bytes_accessed=0, transcendentals=0),
        compiler_params=pltpu.CompilerParams(vmem_limit_bytes=GRANT),
        name="number",
    )()
    taken = {
        "normal": wall_normal, "ref": sample_ref, "relax": relax.reshape(1, 27),
        "solid": solid, "scell": stencil_cell, "sweight": stencil_weight,
    }
    passed = [taken[name] for name in THROUGH]
    cells, *passed = pl.pallas_call(
        live_kernel,
        out_shape=[jax.ShapeDtypeStruct(v.shape, v.dtype) for v in (number, *passed)],
        in_specs=[VMEM, pl.BlockSpec(memory_space=pltpu.SMEM)] + [VMEM] * (1 + len(passed)),
        out_specs=[VMEM] * (1 + len(passed)),
        compiler_params=pltpu.CompilerParams(vmem_limit_bytes=GRANT),
        name="live",
    )(number, wall_count, wall_cell, *passed)
    taken.update(zip(THROUGH, passed))
    y_even, y_odd, samples, state, early, maps = pl.pallas_call(
        lambda *refs: first_kernel(*refs, gy="gy"),
        out_shape=[
            jax.ShapeDtypeStruct(face, f32),
            jax.ShapeDtypeStruct(face, f32),
            jax.ShapeDtypeStruct((lines, LANES), f32),
            jax.ShapeDtypeStruct((PLANES, *block), f32),
            jax.ShapeDtypeStruct((11, ROWS, LANES), f32),
            jax.ShapeDtypeStruct((3, *block), f32),
        ],
        in_specs=[VMEM] * 8,
        out_specs=[VMEM] * 6,
        compiler_params=pltpu.CompilerParams(vmem_limit_bytes=GRANT),
        name="first",
    )(cells, *taken.values(), populations)

    def swap(value, odd):
        return lax.ppermute(value, "gy", [(i, (((i - odd) ^ 1) + odd) % peers) for i in range(peers)])

    got_far = []
    for n in range(2, peers - 1) if peers != 4 else ():
        got_far.append(lax.ppermute(samples, "gy", [(i, (i + n) % peers) for i in range(peers)]))
    y_odd = swap(y_odd, 1)
    y_even = swap(y_even, 0)
    if peers == 4:
        got_far = [swap(y_odd, 0)]
    ring = [(i, (i + 1) % devices) for i in range(devices)]
    early = lax.ppermute(early, "gx", ring)
    plus, minus, vel, halo = pl.pallas_call(
        lambda *refs: second_kernel(*refs, gy="gy", peers=peers, slots=slots, slots_each=slots_each),
        out_shape=[
            jax.ShapeDtypeStruct((4, ROWS, LANES), f32),
            jax.ShapeDtypeStruct((11, ROWS, LANES), f32),
            jax.ShapeDtypeStruct((3, *block), f32),
            jax.ShapeDtypeStruct((3, ROWS, LANES), f32),
        ],
        in_specs=[VMEM] * (5 + len(got_far)),
        out_specs=[VMEM] * 4,
        compiler_params=pltpu.CompilerParams(vmem_limit_bytes=GRANT),
        name="second",
    )(samples, y_even, y_odd, state, maps, *got_far)
    post, edge = pl.pallas_call(
        lambda *refs: third_kernel(*refs, gy="gy", slots=slots),
        out_shape=[jax.ShapeDtypeStruct(populations.shape, f32), jax.ShapeDtypeStruct((up(20 * size_x), LANES), f32)],
        in_specs=[VMEM] * 5,
        out_specs=[VMEM] * 2,
        compiler_params=pltpu.CompilerParams(vmem_limit_bytes=GRANT),
        name="third",
    )(y_even, y_odd, state, vel, halo)
    from_below = lax.ppermute(plus, "gx", ring)
    from_above = lax.ppermute(minus, "gx", [(i, (i - 1) % devices) for i in range(devices)])
    held = pl.pallas_call(
        inner_kernel,
        out_shape=jax.ShapeDtypeStruct(populations.shape, f32),
        in_specs=[VMEM] * 3,
        out_specs=HBM,
        scratch_shapes=[pltpu.VMEM(populations.shape, f32), pltpu.SemaphoreType.DMA((3,))],
        compiler_params=pltpu.CompilerParams(vmem_limit_bytes=GRANT),
        name="inner",
    )(post, edge, maps)
    return pl.pallas_call(
        outer_kernel,
        out_shape=jax.ShapeDtypeStruct(populations.shape, f32),
        in_specs=[VMEM] * 4 + [HBM],
        out_specs=HBM,
        input_output_aliases={4: 0},
        scratch_shapes=[pltpu.VMEM((18, ROWS, LANES), f32), pltpu.SemaphoreType.DMA((2,))],
        compiler_params=pltpu.CompilerParams(vmem_limit_bytes=GRANT),
        name="outer",
    )(post, early, from_below, from_above, pltpu.with_memory_space_constraint(held, pltpu.HBM))


def solution(mesh):
    return jax.shard_map(
        local,
        mesh=mesh,
        in_specs=(
            P(None, "gx", "gy", None),
            P(),
            P("gx", "gy", None),
            P("gx", "gy", None),
            P("gx", "gy", None),
            P("gx", "gy"),
            P("gx", "gy", None),
            P("gx", "gy", None, None),
            P("gx", "gy", None, None),
        ),
        out_specs=P(None, "gx", "gy", None),
        check_vma=False,
    )
```

```python
import jax
import jax.numpy as jnp
from jax import lax
from jax.experimental import pallas as pl
from jax.experimental.pallas import tpu as pltpu
from jax.sharding import PartitionSpec as P


wall_ratio = (1.0 / 9.0) ** (1.0 / 7.0)
LANES = 128
ROWS = 8
RHO, VEL, PLANES = 27, 28, 31
REF, AXIS, SOLID = 0, 1, 2
FACE = 16
HBM = pl.BlockSpec(memory_space=pltpu.HBM)
VMEM = pl.BlockSpec(memory_space=pltpu.VMEM)
THROUGH = ("normal", "ref", "relax")
COVER = 4 * 10**9
GRANT = 4 * 1024 * 1024


def direction(a, b, c):
    return 9 * a + 3 * b + c


def up(n):
    return -(-n // ROWS) * ROWS


def equilibria(density, velocity, wanted):
    ux, uy, uz = velocity
    rest = density * (1.0 - 1.5 * (ux * ux + uy * uy + uz * uz))
    out = {}
    for i in wanted:
        if i in out:
            continue
        step = (i // 9 - 1, i // 3 % 3 - 1, i % 3 - 1)
        along = None
        for s, u in zip(step, (ux, uy, uz)):
            if s:
                along = (u if s > 0 else -u) if along is None else (along + u if s > 0 else along - u)
        if along is None:
            out[i] = rest
            continue
        linear = density * along
        square = rest + 4.5 * (linear * along)
        out[i] = square + 3.0 * linear
        if 26 - i in wanted:
            out[26 - i] = square - 3.0 * linear
    return out


def along_axes(values, triple):
    for stride in (1, 3, 9):
        fresh = list(values)
        for i in range(27):
            if i // stride % 3 == 0:
                fresh[i], fresh[i + stride], fresh[i + 2 * stride] = triple(
                    values[i], values[i + stride], values[i + 2 * stride]
                )
        values = fresh
    return values


def relaxed(pops, keep):
    single = (1.0 / 6.0, 2.0 / 3.0, 1.0 / 6.0)
    weight = [single[i // 9] * single[i // 3 % 3] * single[i % 3] for i in range(27)]

    def raw(m, z, p):
        s = m + p
        return s + z, p - m, s

    def undo(m0, m1, m2):
        return m2 - m1, m0 - m2, m1 + m2

    moment = along_axes([w * p for w, p in zip(weight, pops)], raw)
    density = moment[0]
    inv = 1.0 / density
    vel = [moment[9] * inv, moment[3] * inv, moment[1] * inv]
    first = [moment[9], moment[3], moment[1]]
    second = [4.5 * (j * u) for j, u in zip(first, vel)]
    rest = density - (1.0 / 3.0) * (second[0] + second[1] + second[2])
    mu, nu, ka = (1.0, 0.0, 1.0 / 3.0), (0.0, 1.0 / 3.0, 0.0), (1.0 / 3.0, 0.0, 1.0 / 3.0)
    cross = {}
    kept = []
    for i in range(27):
        p = (i // 9, i // 3 % 3, i % 3)
        eq = None
        terms = [(mu[p[0]] * mu[p[1]] * mu[p[2]], rest)]
        for d in range(3):
            o, q = [e for e in range(3) if e != d]
            terms.append((3.0 * nu[p[d]] * mu[p[o]] * mu[p[q]], first[d]))
            terms.append((ka[p[d]] * mu[p[o]] * mu[p[q]], second[d]))
            factor = 9.0 * nu[p[o]] * nu[p[q]] * mu[p[d]]
            if factor:
                if d not in cross:
                    cross[d] = first[o] * vel[q]
                terms.append((factor, cross[d]))
        for f, t in terms:
            if f:
                t = t if abs(f - 1.0) < 1e-12 else f * t
                eq = t if eq is None else eq + t
        dev = moment[i] if eq is None else moment[i] - eq
        kept.append(keep[i] * dev)
    back = (3.0, 1.5, 3.0)
    kept = along_axes(kept, undo)
    kept = [back[i // 9] * back[i // 3 % 3] * back[i % 3] * k for i, k in enumerate(kept)]
    return density, vel, kept


def lanes_of(table, index):
    return jnp.take_along_axis(table, index, axis=1, mode="promise_in_bounds")


def number_kernel(out):
    out[...] = lax.broadcasted_iota(jnp.int32, out.shape, 1)


def live_kernel(number, count, cell, *rest):
    half = (len(rest) - 1) // 2
    rest[half][...] = jnp.where(number[...] < count[0, 0], cell[0], -1)
    for source, target in zip(rest[:half], rest[half + 1 :]):
        target[...] = source[...]


def cell_kernel(relax, pop, scell, sweight, state_o, sample_o):
    size_x, slots = pop.shape[1], scell.shape[-1]
    rates = [1.0 - jnp.broadcast_to(relax[0:1, i : i + 1], (ROWS, LANES)) for i in range(27)]
    velocity = []
    for x in range(size_x):
        density, vel, kept = relaxed([pop[i, x] for i in range(27)], rates)
        velocity.append(vel)
        for i in range(27):
            state_o[i, x] = kept[i]
        state_o[RHO, x] = density
        for d in range(3):
            state_o[VEL + d, x] = vel[d]
    sub = lax.broadcasted_iota(jnp.int32, (ROWS, LANES), 0)
    for t in range(slots // LANES):
        cells = scell[0, 0, :, t * LANES : (t + 1) * LANES]
        weights = sweight[0, 0, :, t * LANES : (t + 1) * LANES]
        row, z = cells // LANES, cells % LANES
        low = jnp.broadcast_to(z[0:1], (ROWS, LANES))
        other = z != low
        high = jnp.max(jnp.where(other, z, 0), axis=0, keepdims=True)
        high = jnp.broadcast_to(high, (ROWS, LANES))
        w_high = jnp.where(other, weights, 0.0)
        w_low = weights - w_high
        total = [None] * 3
        for x in range(size_x):
            a_low = jnp.zeros((ROWS, LANES), jnp.float32)
            a_high = a_low
            for k in range(8):
                hit = jnp.broadcast_to(row[k : k + 1], (ROWS, LANES)) == sub + x * ROWS
                a_low += jnp.where(hit, jnp.broadcast_to(w_low[k : k + 1], (ROWS, LANES)), 0.0)
                a_high += jnp.where(hit, jnp.broadcast_to(w_high[k : k + 1], (ROWS, LANES)), 0.0)
            for d in range(3):
                part = a_low * lanes_of(velocity[x][d], low) + a_high * lanes_of(velocity[x][d], high)
                total[d] = part if total[d] is None else total[d] + part
        for d in range(3):
            r = d * (slots // LANES) + t
            sample_o[r : r + 1, :] = jnp.sum(total[d], axis=0, keepdims=True)


def face_kernel(cell, normal, ref, solid, state, sample, even_o, odd_o, early_o, map_o, *, gy):
    size_x, walls = solid.shape[0], cell.shape[-1]
    row = jnp.where(cell[...] < 0, -1, cell[...] // LANES)
    z = cell[...] % LANES
    low = (ref[0] % LANES + 1).astype(jnp.float32)
    high = (ref[0] // LANES * 4 + normal[0] // 2).astype(jnp.float32)
    height = size_x * ROWS
    at = lax.broadcasted_iota(jnp.int32, (height, walls), 0) == jnp.broadcast_to(row, (height, walls))
    left = jnp.concatenate(
        [jnp.where(at, jnp.broadcast_to(v, (height, walls)), 0.0) for v in (low, high)], axis=0
    ).astype(jnp.bfloat16)
    hot = lax.broadcasted_iota(jnp.int32, (LANES, walls), 0) == jnp.broadcast_to(z, (LANES, walls))
    hot = jnp.where(hot, 1.0, 0.0).astype(jnp.bfloat16)
    dense = lax.dot_general(left, hot, (((1,), (1,)), ((), ())), preferred_element_type=jnp.float32)
    for x in range(size_x):
        low = dense[x * ROWS : (x + 1) * ROWS].astype(jnp.int32)
        high = dense[height + x * ROWS : height + (x + 1) * ROWS].astype(jnp.int32)
        map_o[REF, x] = ((high // 4) * LANES + low - 1).astype(jnp.float32)
        map_o[AXIS, x] = (high % 4).astype(jnp.float32)
        map_o[SOLID, x] = solid[x].astype(jnp.float32)
    for n in range(9):
        early_o[n] = state[18 + n, size_x - 1]
    early_o[9] = state[RHO, size_x - 1]
    early_o[10] = map_o[SOLID, size_x - 1]
    base = sample.shape[0]
    even_o[:base, :] = sample[...]
    parity = lax.axis_index(gy) % 2
    faces = []
    for b, y in ((2, ROWS - 1), (0, 0)):
        planes = [(state, direction(a, b, c)) for a in range(3) for c in range(3)]
        planes += [(state, n) for n in range(RHO, PLANES)] + [(map_o, n) for n in range(3)]
        faces.append([array[plane, x, y : y + 1, :] for array, plane in planes for x in range(size_x)])
    for n, (above, below) in enumerate(zip(*faces)):
        even_o[base + n : base + n + 1, :] = jnp.where(parity == 0, above, below)
        odd_o[n : n + 1, :] = jnp.where(parity == 0, below, above)


def first_kernel(
    cells, normal, ref, relax, solid, scell, sweight, pop, even_o, odd_o, sample_o, state_o, early_o, map_o, *, gy
):
    cell_kernel(relax, pop, scell, sweight, state_o, sample_o)
    face_kernel(cells, normal, ref, solid, state_o, sample_o, even_o, odd_o, early_o, map_o, gy=gy)


def owners(own, y_even, s_odd, far, gy, peers):
    me = lax.axis_index(gy)
    below, above = (me + peers - 1) % peers, (me + 1) % peers
    even = me % 2 == 0
    tables = [(own, me), (y_even, jnp.where(even, above, below)), (s_odd, jnp.where(even, below, above))]
    tables += [(table, (me + peers - (n + 2)) % peers) for n, table in enumerate(far)]
    return tables, me, below, above


def walled(tables, block, width, slots_each, ref, axis, vel):
    index = jnp.maximum(ref, 0)
    source = index // slots_each
    lane = block(lambda p: p * slots_each % LANES) + index % slots_each
    out = []
    for d in range(3):
        picked = jnp.zeros(ref.shape, jnp.float32)
        for table, who in tables:

            def line(p):
                return jnp.broadcast_to(table[pl.ds(d * width + p * slots_each // LANES, 1), :], (ROWS, LANES))

            picked = jnp.where(source == who, lanes_of(block(line), lane), picked)
        tangential = jnp.where(axis == d, 0.0, wall_ratio * picked)
        out.append(jnp.where(ref >= 0, tangential, vel[d]))
    return out


def beside(y_even, y_odd, gy, base, size_x):
    even = lax.axis_index(gy) % 2 == 0
    sub = lax.broadcasted_iota(jnp.int32, (ROWS, LANES), 0)

    def plane(n):
        got = (y_odd[pl.ds(n * size_x, size_x), :], y_even[pl.ds(base + n * size_x, size_x), :])
        tile = None
        for side in range(2):
            picked = jnp.where(even, got[side], got[1 - side])
            for x in range(size_x):
                row = jnp.broadcast_to(picked[x : x + 1], (ROWS, LANES))
                tile = row if tile is None else jnp.where(sub == side * size_x + x, row, tile)
        return tile

    return plane, sub


def second_kernel(own, y_even, y_odd, s_odd, state, maps, *rest, gy, peers, slots, slots_each):
    far, (plus_o, minus_o, vel_o, halo_o) = rest[: peers - 3], rest[peers - 3 :]
    size_x, width = maps.shape[1], slots // LANES
    tables, me, below, above = owners(own, y_even, s_odd, far, gy, peers)
    plane, sub = beside(y_even, y_odd, gy, up(3 * width), size_x)
    first_side = sub < size_x
    for x in range(size_x):
        ref, axis = maps[REF, x].astype(jnp.int32), maps[AXIS, x].astype(jnp.int32)
        vel = [state[VEL + d, x] for d in range(3)]
        vel = walled(tables, lambda f: f(me), width, slots_each, ref, axis, vel)
        for d in range(3):
            vel_o[d, x] = vel[d]
            if x == size_x - 1:
                plus_o[d] = vel[d]
        if x == 0:
            eq = equilibria(state[RHO, x], vel, range(9))
            for i in range(9):
                minus_o[i] = state[i, x] + eq[i]
            minus_o[9] = maps[SOLID, x]
    ref, axis = plane(13).astype(jnp.int32), plane(14).astype(jnp.int32)
    vel = [plane(10 + d) for d in range(3)]
    vel = walled(tables, lambda f: jnp.where(first_side, f(below), f(above)), width, slots_each, ref, axis, vel)
    vel[1] = jnp.where(first_side, vel[1], -vel[1])
    for d in range(3):
        halo_o[d] = vel[d]
    eq = equilibria(plane(9), vel, [direction(a, 2, c) for a in (0, 2) for c in range(3)])
    solid = plane(15)
    for o, a, x, last in ((plus_o, 2, size_x - 1, 3), (minus_o, 0, 0, 10)):
        corner = [plane(3 * a + c) + eq[direction(a, 2, c)] for c in range(3)] + [solid]
        for side in range(2):
            r = side * size_x + x
            for n in range(4):
                o[last, side * 4 + n : side * 4 + n + 1, :] = corner[n][r : r + 1]


def third_kernel(y_even, y_odd, state, vel, halo, post_o, edge_o, *, gy, slots):
    size_x = post_o.shape[1]
    plane, _ = beside(y_even, y_odd, gy, up(3 * (slots // LANES)), size_x)
    for x in range(size_x):
        eq = equilibria(state[RHO, x], [vel[d, x] for d in range(3)], range(27))
        for i in range(27):
            post_o[i, x] = state[i, x] + eq[i]
    wanted = [direction(a, 2, c) for a in range(3) for c in range(3)]
    eq = equilibria(plane(9), [halo[d] for d in range(3)], wanted)
    for n, value in enumerate([plane(n) + eq[i] for n, i in enumerate(wanted)] + [plane(15)]):
        for side in range(2):
            r = (side * 10 + n) * size_x
            edge_o[r : r + size_x, :] = value[side * size_x : (side + 1) * size_x]


def shifted(tile, row, step_y):
    if step_y == 0:
        return tile
    sub = lax.broadcasted_iota(jnp.int32, (ROWS, LANES), 0)
    rolled = pltpu.roll(tile, step_y % ROWS, 0)
    return jnp.where(sub == (0 if step_y > 0 else ROWS - 1), jnp.broadcast_to(row, (ROWS, LANES)), rolled)


def along_z(tile, c):
    return tile if c == 1 else pltpu.roll(tile, (c - 1) % LANES, 1)


def inner_kernel(post, edge, maps, out_h, out, sems):
    size_x = post.shape[1]
    copies = []
    for a in (1, 2, 0):
        first, last = max(a - 1, 0), size_x + min(a - 1, 0)
        for b in range(3):
            side = 0 if b == 2 else 1
            for x in range(first, last):
                q = x - (a - 1)

                def row(n):
                    r = (side * 10 + n) * size_x + q
                    return edge[r : r + 1, :]

                wall = shifted(maps[SOLID, q], row(9), b - 1)
                for c in range(3):
                    i = direction(a, b, c)
                    moved = along_z(shifted(post[i, q], row(3 * a + c), b - 1), c)
                    out[i, x] = jnp.where(along_z(wall, c) > 0.5, post[26 - i, x], moved)
        part = (pl.ds(9 * a, 9), pl.ds(first, last - first))
        copy = pltpu.make_async_copy(out.at[part], out_h.at[part], sems.at[a])
        copy.start()
        copies.append(copy)
    for copy in copies:
        copy.wait()


def outer_kernel(post, early, below, above, held_h, out_h, out, sems):
    del held_h
    size_x = post.shape[1]
    copies = []
    for a, x in ((0, size_x - 1), (2, 0)):
        if a == 0:
            tiles, solid, corner = [above[n] for n in range(9)], above[9], above[10]
        else:
            eq = equilibria(early[9], [below[d] for d in range(3)], range(18, 27))
            tiles, solid, corner = [early[n] + eq[18 + n] for n in range(9)], early[10], below[3]
        for b in range(3):
            side = 0 if b == 2 else 1
            wall = shifted(solid, corner[side * 4 + 3 : side * 4 + 4], b - 1)
            for c in range(3):
                i = direction(a, b, c)
                moved = shifted(tiles[3 * b + c], corner[side * 4 + c : side * 4 + c + 1], b - 1)
                moved = along_z(moved, c)
                out[i % 9 + 9 * (a // 2)] = jnp.where(along_z(wall, c) > 0.5, post[26 - i, x], moved)
            held, taken = out.at[pl.ds(9 * (a // 2) + 3 * b, 3)], out_h.at[pl.ds(9 * a + 3 * b, 3), x]
            copies.append(pltpu.make_async_copy(held, taken, sems.at[len(copies)]))
            copies[-1].start()
    for copy in copies:
        copy.wait()


def local(
    populations, relax, solid, wall_cell, wall_normal, wall_count, sample_ref, stencil_cell, stencil_weight
):
    _, size_x, size_y, size_z = populations.shape
    walls, slots = wall_cell.shape[-1], stencil_cell.shape[-1]
    devices, peers = lax.axis_size("gx"), lax.axis_size("gy")
    slots_each = slots // peers
    if (size_y, size_z) != (ROWS, LANES) or walls % LANES or slots % LANES:
        raise ValueError("unsupported block")
    if LANES % slots_each or peers % 2 or peers < 4 or 2 * size_x > ROWS:
        raise ValueError("unsupported mesh")
    f32 = jnp.float32
    lines = up(3 * (slots // LANES))
    face = (lines + FACE * size_x, LANES)
    block = (size_x, ROWS, LANES)
    number = pl.pallas_call(
        number_kernel,
        out_shape=jax.ShapeDtypeStruct((1, walls), jnp.int32),
        out_specs=VMEM,
        cost_estimate=pl.CostEstimate(flops=COVER, bytes_accessed=0, transcendentals=0),
        compiler_params=pltpu.CompilerParams(vmem_limit_bytes=GRANT),
        name="number",
    )()
    taken = {
        "normal": wall_normal, "ref": sample_ref, "relax": relax.reshape(1, 27),
        "solid": solid, "scell": stencil_cell, "sweight": stencil_weight,
    }
    passed = [taken[name] for name in THROUGH]
    cells, *passed = pl.pallas_call(
        live_kernel,
        out_shape=[jax.ShapeDtypeStruct(v.shape, v.dtype) for v in (number, *passed)],
        in_specs=[VMEM, pl.BlockSpec(memory_space=pltpu.SMEM)] + [VMEM] * (1 + len(passed)),
        out_specs=[VMEM] * (1 + len(passed)),
        compiler_params=pltpu.CompilerParams(vmem_limit_bytes=GRANT),
        name="live",
    )(number, wall_count, wall_cell, *passed)
    taken.update(zip(THROUGH, passed))
    y_even, y_odd, samples, state, early, maps = pl.pallas_call(
        lambda *refs: first_kernel(*refs, gy="gy"),
        out_shape=[
            jax.ShapeDtypeStruct(face, f32),
            jax.ShapeDtypeStruct((FACE * size_x, LANES), f32),
            jax.ShapeDtypeStruct((lines, LANES), f32),
            jax.ShapeDtypeStruct((PLANES, *block), f32),
            jax.ShapeDtypeStruct((11, ROWS, LANES), f32),
            jax.ShapeDtypeStruct((3, *block), f32),
        ],
        in_specs=[VMEM] * 8,
        out_specs=[VMEM] * 6,
        compiler_params=pltpu.CompilerParams(vmem_limit_bytes=GRANT),
        name="first",
    )(cells, *taken.values(), populations)

    def swap(value, odd):
        return lax.ppermute(value, "gy", [(i, (((i - odd) ^ 1) + odd) % peers) for i in range(peers)])

    got_far = []
    for n in range(2, peers - 1) if peers != 4 else ():
        got_far.append(lax.ppermute(samples, "gy", [(i, (i + n) % peers) for i in range(peers)]))
    s_odd = swap(samples, 1)
    y_odd = swap(y_odd, 1)
    y_even = swap(y_even, 0)
    if peers == 4:
        got_far = [swap(s_odd, 0)]
    ring = [(i, (i + 1) % devices) for i in range(devices)]
    early = lax.ppermute(early, "gx", ring)
    plus, minus, vel, halo = pl.pallas_call(
        lambda *refs: second_kernel(*refs, gy="gy", peers=peers, slots=slots, slots_each=slots_each),
        out_shape=[
            jax.ShapeDtypeStruct((4, ROWS, LANES), f32),
            jax.ShapeDtypeStruct((11, ROWS, LANES), f32),
            jax.ShapeDtypeStruct((3, *block), f32),
            jax.ShapeDtypeStruct((3, ROWS, LANES), f32),
        ],
        in_specs=[VMEM] * (6 + len(got_far)),
        out_specs=[VMEM] * 4,
        compiler_params=pltpu.CompilerParams(vmem_limit_bytes=GRANT),
        name="second",
    )(samples, y_even, y_odd, s_odd, state, maps, *got_far)
    post, edge = pl.pallas_call(
        lambda *refs: third_kernel(*refs, gy="gy", slots=slots),
        out_shape=[jax.ShapeDtypeStruct(populations.shape, f32), jax.ShapeDtypeStruct((up(20 * size_x), LANES), f32)],
        in_specs=[VMEM] * 5,
        out_specs=[VMEM] * 2,
        compiler_params=pltpu.CompilerParams(vmem_limit_bytes=GRANT),
        name="third",
    )(y_even, y_odd, state, vel, halo)
    from_below = lax.ppermute(plus, "gx", ring)
    from_above = lax.ppermute(minus, "gx", [(i, (i - 1) % devices) for i in range(devices)])
    held = pl.pallas_call(
        inner_kernel,
        out_shape=jax.ShapeDtypeStruct(populations.shape, f32),
        in_specs=[VMEM] * 3,
        out_specs=HBM,
        scratch_shapes=[pltpu.VMEM(populations.shape, f32), pltpu.SemaphoreType.DMA((3,))],
        compiler_params=pltpu.CompilerParams(vmem_limit_bytes=GRANT),
        name="inner",
    )(post, edge, maps)
    return pl.pallas_call(
        outer_kernel,
        out_shape=jax.ShapeDtypeStruct(populations.shape, f32),
        in_specs=[VMEM] * 4 + [HBM],
        out_specs=HBM,
        input_output_aliases={4: 0},
        scratch_shapes=[pltpu.VMEM((18, ROWS, LANES), f32), pltpu.SemaphoreType.DMA((6,))],
        compiler_params=pltpu.CompilerParams(vmem_limit_bytes=GRANT),
        name="outer",
    )(post, early, from_below, from_above, pltpu.with_memory_space_constraint(held, pltpu.HBM))


def solution(mesh):
    return jax.shard_map(
        local,
        mesh=mesh,
        in_specs=(
            P(None, "gx", "gy", None),
            P(),
            P("gx", "gy", None),
            P("gx", "gy", None),
            P("gx", "gy", None),
            P("gx", "gy"),
            P("gx", "gy", None),
            P("gx", "gy", None, None),
            P("gx", "gy", None, None),
        ),
        out_specs=P(None, "gx", "gy", None),
        check_vma=False,
    )
```
